32 devices in a mesh: dz: 4 (over z), dy: 2 (over y), dx: 4 (over x, core).
Axes of the slice: x: 2, y: 2, z: 4, core: 2. Of those that a mesh axis runs over, the one named last changes fastest.
Arguments:
- g_emb: float32 [32, 512, 512], P(('dz', 'dy', 'dx'))
- g_attn: float32 [32, 1, 4, 512, 512], P(('dz', 'dy', 'dx'))
- g_in: float32 [32, 1, 512, 2048], P(('dz', 'dy', 'dx'))
- g_out: float32 [32, 1, 2048, 512], P(('dz', 'dy', 'dx'))
- g_vecd: float32 [32, 1, 9, 512], P(('dz', 'dy', 'dx'))
- g_vecf: float32 [32, 1, 2048], P(('dz', 'dy', 'dx'))
- opt_m: float32 [3416064], P(('dz', 'dy', 'dx'))
- opt_v: float32 [3416064], P(('dz', 'dy', 'dx'))
- master: float32 [3416064], P(('dz', 'dy', 'dx'))
- tok_ids: int32 [524288], P(('dz', 'dy', 'dx'))
- act_in: bfloat16 [524288, 512], P(('dz', 'dy', 'dx'))
Outputs:
- output 1: float32 [3416064], P(('dz', 'dy', 'dx'))
- output 2: float32 [3416064], P(('dz', 'dy', 'dx'))
- output 3: float32 [3416064], P(('dz', 'dy', 'dx'))
- output 4: bfloat16 [512, 512], replicated
- output 5: bfloat16 [1, 4, 512, 512], replicated
- output 6: bfloat16 [1, 512, 2048], replicated
- output 7: bfloat16 [1, 2048, 512], replicated
- output 8: bfloat16 [1, 9, 512], replicated
- output 9: bfloat16 [1, 2048], replicated
- output 10: bfloat16 [524288, 512], P(('dz', 'dy', 'dx'))
All inputs are finite; a program needn't handle non-finite values.
Results may differ from the reference program's by a relative error of at most 0.001.
Values are sent between devices in bfloat16 or wider.
A program may use at most 1 GiB of HBM per device.

```python
import math
import jax
import jax.numpy as jnp
from jax import lax

D = 512
FF = 2048
LAYERS = 1
VOCAB = 512
TOKENS_DEV = 16384
DEVICES = 32
ADAM_STEP = 2

LEARN_RATE = 0.002
BETA_ONE = 0.9
BETA_TWO = 0.95
ADAM_EPS = 1e-8
PARAM_COUNT = VOCAB * D + LAYERS * (4 * D * D + 2 * D * FF + 9 * D + FF)
PADDED_COUNT = -(-PARAM_COUNT // (128 * DEVICES)) * (128 * DEVICES)
TENSOR_SHAPES = [(VOCAB, D), (LAYERS, 4, D, D), (LAYERS, D, FF), (LAYERS, FF, D), (LAYERS, 9, D), (LAYERS, FF)]
ARG_NAMES = ["g_emb", "g_attn", "g_in", "g_out", "g_vecd", "g_vecf"]


def setup_inputs(seed: int = 0) -> dict:
    rand_keys = jax.random.split(jax.random.key(seed), 12)
    dev_scale = jax.random.uniform(rand_keys[0], (DEVICES,), jnp.float32, 0.5, 1.5) * math.sqrt(DEVICES)
    inputs = {}
    for tensor_index, tensor_shape in enumerate(TENSOR_SHAPES):
        grad_noise = jax.random.normal(rand_keys[1 + tensor_index], (DEVICES,) + tensor_shape, jnp.float32)
        inputs[ARG_NAMES[tensor_index]] = grad_noise * dev_scale.reshape((DEVICES,) + (1,) * len(tensor_shape))
    weight_scales = [D ** -0.5, D ** -0.5, D ** -0.5, FF ** -0.5, 0.2, 0.3]
    scale_parts = [jnp.full((math.prod(tensor_shape),), weight_scale, jnp.float32) for tensor_shape, weight_scale in zip(TENSOR_SHAPES, weight_scales)]
    scale_parts.append(jnp.full((PADDED_COUNT - PARAM_COUNT,), 0.1, jnp.float32))
    m_noise = jax.random.normal(rand_keys[7], (PADDED_COUNT,), jnp.float32)
    v_noise = jax.random.normal(rand_keys[8], (PADDED_COUNT,), jnp.float32)
    w_noise = jax.random.normal(rand_keys[9], (PADDED_COUNT,), jnp.float32)
    inputs["opt_m"] = 0.1 * m_noise
    inputs["opt_v"] = 0.05 * (v_noise * v_noise + 0.25)
    inputs["master"] = w_noise * jnp.concatenate(scale_parts)
    tok_ids = jax.random.randint(rand_keys[10], (DEVICES * TOKENS_DEV,), 0, VOCAB, jnp.int32)
    inputs["tok_ids"] = tok_ids.at[0].set(0).at[1].set(VOCAB - 1)
    inputs["act_in"] = jax.random.normal(rand_keys[11], (DEVICES * TOKENS_DEV, D), jnp.float32).astype(jnp.bfloat16)
    return inputs


def ffn_block(wb_emb, w_in, b_in, w_out, b_out, tok_ids, act_in):
    emb_rows = jnp.take(wb_emb, tok_ids, axis=0).astype(jnp.float32)
    hidden = (emb_rows * math.sqrt(D) + act_in.astype(jnp.float32)).astype(jnp.bfloat16)
    pre_act = jnp.dot(hidden, w_in, preferred_element_type=jnp.float32) + b_in.astype(jnp.float32)
    inner_act = jax.nn.gelu(pre_act, approximate=True).astype(jnp.bfloat16)
    return (jnp.dot(inner_act, w_out, preferred_element_type=jnp.float32) + b_out.astype(jnp.float32)).astype(jnp.bfloat16)


def reference(g_emb, g_attn, g_in, g_out, g_vecd, g_vecf, opt_m, opt_v, master, tok_ids, act_in):
    grad_list = [g_emb, g_attn, g_in, g_out, g_vecd, g_vecf]
    flat_grad = jnp.concatenate([jnp.sum(grad_arr, axis=0).reshape(-1) for grad_arr in grad_list]) / DEVICES
    flat_grad = jnp.pad(flat_grad, (0, PADDED_COUNT - PARAM_COUNT))
    m_new = BETA_ONE * opt_m + (1.0 - BETA_ONE) * flat_grad
    v_new = BETA_TWO * opt_v + (1.0 - BETA_TWO) * flat_grad * flat_grad
    m_hat = m_new / (1.0 - BETA_ONE ** ADAM_STEP)
    v_hat = v_new / (1.0 - BETA_TWO ** ADAM_STEP)
    w_new = master - LEARN_RATE * m_hat / (jnp.sqrt(v_hat) + ADAM_EPS)
    w_half = w_new.astype(jnp.bfloat16)
    pieces = []
    offset = 0
    for tensor_shape in TENSOR_SHAPES:
        elem_count = math.prod(tensor_shape)
        pieces.append(w_half[offset:offset + elem_count].reshape(tensor_shape))
        offset = offset + elem_count
    wb_emb, wb_attn, wb_in, wb_out, wb_vecd, wb_vecf = pieces
    tok_blocks = tok_ids.reshape(DEVICES, TOKENS_DEV)
    act_blocks = act_in.reshape(DEVICES, TOKENS_DEV, D)

    def token_block(tok_pair):
        return ffn_block(wb_emb, wb_in[0], wb_vecf[0], wb_out[0], wb_vecd[0, 8], tok_pair[0], tok_pair[1])

    y_blocks = lax.map(token_block, (tok_blocks, act_blocks))
    y_out = y_blocks.reshape(DEVICES * TOKENS_DEV, D)
    return (m_new, v_new, w_new, wb_emb, wb_attn, wb_in, wb_out, wb_vecd, wb_vecf, y_out)
```

```python
import functools
import math

import jax
import jax.numpy as jnp
from jax import lax
from jax.experimental import pallas as pl
from jax.experimental.pallas import tpu as pltpu
from jax.sharding import PartitionSpec as P

LEARN_RATE = 0.002
BETA_ONE = 0.9
BETA_TWO = 0.95
ADAM_EPS = 1e-8
ADAM_STEP = 2
AXES = ("dz", "dy", "dx")
GRAD_RANKS = (3, 5, 4, 4, 4, 3)
MESH = pl.DeviceIdType.MESH
F32, BF16 = jnp.float32, jnp.bfloat16

D, FF, VOCAB = 512, 2048, 512
ROWS = 26688
SHARD = 834
WIN = 840
WROWS = 848
TENSORS = ((0, 512, 512), (2048, 2048, 512), (10240, 512, 2048), (18432, 2048, 512))
VEC_ROW = 26624
COLORS = (
    ((0, 1, 2, 3), (0, 208), (0, 208)),
    ((1, 2, 3, 0), (208, 208), (208, 208)),
    ((2, 3, 0, 1), (416, 208), (416, 208)),
    ((3, 0, 1, 2), (624, 216), (624, 224)),
)
NC = len(COLORS)


def adam_update(grad_vals, opt_m, opt_v, master):
    m_new = BETA_ONE * opt_m + (1.0 - BETA_ONE) * grad_vals
    v_new = BETA_TWO * opt_v + (1.0 - BETA_TWO) * grad_vals * grad_vals
    m_hat = m_new / (1.0 - BETA_ONE ** ADAM_STEP)
    v_hat = v_new / (1.0 - BETA_TWO ** ADAM_STEP)
    w_new = master - LEARN_RATE * m_hat / (jnp.sqrt(v_hat) + ADAM_EPS)
    return m_new, v_new, w_new


def window_start(s):
    return (s // 4) * 3336 + (s % 4) * 832


def comm_kernel(ge, ga, gi, go, gv, m_in, v_in, w_in, m_out, v_out, w_out, wg_out,
                ne, na, ni, no, flat, acc, r0, r1, r2, r3, r4, ms, vs, ws, wg,
                ld_sem, mvw_sem, s0_s, s0_r, rs_s, rs_r, ag_s, ag_r, pc_s, pc_r, out_sem):
    z, y, xc = lax.axis_index("dz"), lax.axis_index("dy"), lax.axis_index("dx")
    x, c = xc // 2, xc % 2
    b1, b0 = z // 2, z % 2
    g0 = (b0 + b1) % 2
    bits = (b1, g0, y, x)
    peer = (z, y, 2 * x + 1 - c)
    partner = ((3 - z, y, xc), (2 * b1 + 1 - b0, y, xc), (z, 1 - y, xc), (z, y, 2 * (1 - x) + c))

    native = (ne, na, ni, no)
    loads = []
    n_load = 0
    for t, (src, dst, (base, rows, cols)) in enumerate(zip((ge, ga, gi, go), native, TENSORS)):
        chunk = 131072 // cols
        for r in range(0, rows, chunk):
            cp = pltpu.make_async_copy(src.at[pl.ds(r, chunk)], dst.at[pl.ds(r, chunk)], ld_sem.at[n_load])
            cp.start()
            loads.append((cp, t, r, chunk, base + (r + chunk) * cols // 128))
            n_load += 1
    vec_cp = pltpu.make_async_copy(gv, flat.at[pl.ds(VEC_ROW, 64)], ld_sem.at[n_load])
    vec_cp.start()
    mvw = []
    for i, (a, b) in enumerate(((m_in, ms), (v_in, vs), (w_in, ws))):
        cp = pltpu.make_async_copy(a, b, mvw_sem.at[i])
        cp.start()
        mvw.append(cp)

    barrier = pltpu.get_barrier_semaphore()
    for dev in (peer,) + partner:
        pl.semaphore_signal(barrier, inc=1, device_id=dev, device_id_type=MESH)
    pl.semaphore_wait(barrier, 5)

    s0 = []

    def send0(i):
        start = pl.multiple_of(window_start(2 * i + 1 - c), 8)
        cp = pltpu.make_async_remote_copy(flat.at[pl.ds(start, WIN)], r0.at[i], s0_s.at[i], s0_r.at[i],
                                          device_id=peer, device_id_type=MESH)
        cp.start()
        s0.append(cp)

    vec_cp.wait()
    for cp, t, r, chunk, end in loads:
        cp.wait()
        base, _, cols = TENSORS[t]
        lanes = cols // 128

        def group(g, carry, t=t, r=r, base=base, lanes=lanes):
            row = pl.multiple_of(r + g * 8, 8)
            out = base + row * lanes
            for j in range(lanes):
                flat[pl.ds(out + j, 8, stride=lanes), :] = native[t][pl.ds(row, 8), j * 128:(j + 1) * 128]
            return carry

        lax.fori_loop(0, chunk // 8, group, 0, unroll=4 if lanes == 4 else 1)
        if end == VEC_ROW:
            end = ROWS
        while len(s0) < 16 and window_start(2 * len(s0) + 1) + WIN <= end:
            send0(len(s0))

    def slot(i):
        zz = i // 4
        return (zz // 2, (zz % 2 + zz // 2) % 2, (i // 2) % 2, i % 2)

    for i in range(16):
        s0[i].wait_recv()
        start = pl.multiple_of(window_start(2 * i + c), 8)
        acc[slot(i)] = flat[pl.ds(start, WIN), :] + r0[i]

    recv = (r1, r2, r3, r4)
    full = pl.ds(0, 2)

    def rs_copy(k, t):
        order, (row, n), _ = COLORS[k]
        idx = [full] * 4
        for d in order[:t]:
            idx[d] = bits[d]
        idx[order[t]] = 1 - bits[order[t]]
        dst = recv[t].at[(full,) * (3 - t) + (pl.ds(row, n),)]
        return pltpu.make_async_remote_copy(acc.at[tuple(idx) + (pl.ds(row, n),)], dst, rs_s.at[k, t], rs_r.at[k, t],
                                            device_id=partner[order[t]], device_id_type=MESH)

    def rs_add(k, t):
        order, (row, n), _ = COLORS[k]
        idx = [None] * 4
        for d in order[:t + 1]:
            idx[d] = bits[d]
        rest = [d for d in range(4) if idx[d] is None]
        for combo in range(2 ** len(rest)):
            sub = tuple((combo >> (len(rest) - 1 - j)) & 1 for j in range(len(rest)))
            for j, d in enumerate(rest):
                idx[d] = sub[j]
            acc[tuple(idx) + (pl.ds(row, n),)] += recv[t][sub + (pl.ds(row, n),)]

    rs = {}
    for k in range(NC):
        rs[k, 0] = rs_copy(k, 0)
        rs[k, 0].start()
    for t in range(4):
        for k in range(NC):
            rs[k, t].wait_recv()
            rs_add(k, t)
            if t < 3:
                rs[k, t + 1] = rs_copy(k, t + 1)
                rs[k, t + 1].start()

    for cp in mvw:
        cp.wait()
    q = 2 * x + c
    for case in range(4):
        @pl.when(q == case)
        def _():
            grad = acc[bits + (pl.ds(2 * case, SHARD),)] / 32.0
            m_new, v_new, w_new = adam_update(grad, ms[...], vs[...], ws[...])
            ms[...] = m_new
            vs[...] = v_new
            ws[...] = w_new
            wg[(c,) + bits + (pl.ds(SHARD - 2, 16),)] = jnp.zeros((16, 128), BF16)
            wg[(c,) + bits + (pl.ds(0, SHARD),)] = w_new.astype(BF16)
    outs = []
    for i, (a, b) in enumerate(((ms, m_out), (vs, v_out), (ws, w_out))):
        cp = pltpu.make_async_copy(a, b, out_sem.at[i])
        cp.start()
        outs.append(cp)

    def ag_idx(k, t, mine):
        order = COLORS[k][0]
        idx = [full] * 4
        for d in order[:t]:
            idx[d] = bits[d]
        if t < 4:
            idx[order[t]] = bits[order[t]] if mine else 1 - bits[order[t]]
        return (c,) + tuple(idx) + (pl.ds(*COLORS[k][2]),)

    def ag_copy(k, t):
        ref = wg.at[ag_idx(k, t, True)]
        return pltpu.make_async_remote_copy(ref, ref, ag_s.at[k, t], ag_r.at[k, t],
                                            device_id=partner[COLORS[k][0][t]], device_id_type=MESH)

    def pc_copy(k, t):
        ref = wg.at[ag_idx(k, t, False) if t < 4 else (c,) + bits + (pl.ds(*COLORS[k][2]),)]
        return pltpu.make_async_remote_copy(ref, ref, pc_s.at[k, t], pc_r.at[k, t],
                                            device_id=peer, device_id_type=MESH)

    ag, pc = {}, {}
    for k in range(NC):
        ag[k, 3] = ag_copy(k, 3)
        ag[k, 3].start()
    for k in range(NC):
        pc[k, 4] = pc_copy(k, 4)
        pc[k, 4].start()
    for t in (3, 2, 1, 0):
        for k in range(NC):
            ag[k, t].wait_recv()
            if t > 0:
                ag[k, t - 1] = ag_copy(k, t - 1)
                ag[k, t - 1].start()
            pc[k, t] = pc_copy(k, t)
            pc[k, t].start()
    for t in (4, 3, 2, 1, 0):
        for k in range(NC):
            pc[k, t].wait_recv()
    cp = pltpu.make_async_copy(wg, wg_out, out_sem.at[3])
    cp.start()
    outs.append(cp)
    for cp in s0 + list(rs.values()) + list(ag.values()) + list(pc.values()):
        cp.wait_send()
    for cp in outs:
        cp.wait()


def comm(ge, ga, gi, go, gv, m, v, w):
    any_spec = pl.BlockSpec(memory_space=pl.ANY)
    shard = jax.ShapeDtypeStruct((SHARD, 128), F32)
    dma = pltpu.SemaphoreType.DMA
    return pl.pallas_call(
        comm_kernel,
        out_shape=(shard, shard, shard, jax.ShapeDtypeStruct((2, 2, 2, 2, 2, WROWS, 128), BF16)),
        in_specs=[any_spec] * 8,
        out_specs=(any_spec,) * 4,
        scratch_shapes=[
            pltpu.VMEM((512, 512), F32), pltpu.VMEM((2048, 512), F32),
            pltpu.VMEM((512, 2048), F32), pltpu.VMEM((2048, 512), F32),
            pltpu.VMEM((ROWS, 128), F32),
            pltpu.VMEM((2, 2, 2, 2, WIN, 128), F32),
            pltpu.VMEM((16, WIN, 128), F32),
            pltpu.VMEM((2, 2, 2, WIN, 128), F32), pltpu.VMEM((2, 2, WIN, 128), F32),
            pltpu.VMEM((2, WIN, 128), F32), pltpu.VMEM((WIN, 128), F32),
            pltpu.VMEM((SHARD, 128), F32), pltpu.VMEM((SHARD, 128), F32), pltpu.VMEM((SHARD, 128), F32),
            pltpu.VMEM((2, 2, 2, 2, 2, WROWS, 128), BF16),
            dma((32,)), dma((3,)), dma((16,)), dma((16,)),
            dma((NC, 4)), dma((NC, 4)), dma((NC, 4)), dma((NC, 4)), dma((NC, 5)), dma((NC, 5)), dma((4,)),
        ],
        compiler_params=pltpu.CompilerParams(collective_id=0, has_side_effects=True, vmem_limit_bytes=66_000_000),
        name="comm",
    )(ge, ga, gi, go, gv, m, v, w)


def unpack_kernel(wg, we, wa, wi, wo, wv, flat):
    for s in range(32):
        i, core = s // 2, s % 2
        zz = i // 4
        idx = (core, zz // 2, (zz % 2 + zz // 2) % 2, (i // 2) % 2, i % 2)
        flat[pl.ds(s * SHARD, SHARD), :] = wg[idx + (pl.ds(0, SHARD),)].astype(F32)
    for dst, (base, rows, cols) in zip((we, wa, wi, wo), TENSORS):
        lanes = cols // 128

        def group(g, carry, dst=dst, base=base, lanes=lanes):
            row = pl.multiple_of(g * 16, 16)
            for j in range(lanes):
                dst[pl.ds(row, 16), j * 128:(j + 1) * 128] = flat[
                    pl.ds(base + row * lanes + j, 16, stride=lanes), :].astype(BF16)
            return carry

        lax.fori_loop(0, rows // 16, group, 0, unroll=4 if lanes == 4 else 1)
    wv[...] = flat[pl.ds(VEC_ROW, 64), :].astype(BF16)


def unpack(wg):
    vm = pl.BlockSpec(memory_space=pltpu.VMEM)
    shapes = [(512, 512), (2048, 512), (512, 2048), (2048, 512), (64, 128)]
    return pl.pallas_call(
        unpack_kernel,
        out_shape=tuple(jax.ShapeDtypeStruct(s, BF16) for s in shapes),
        in_specs=[vm],
        out_specs=(vm,) * 5,
        scratch_shapes=[pltpu.VMEM((ROWS, 128), F32)],
        compiler_params=pltpu.CompilerParams(vmem_limit_bytes=60_000_000),
        name="unpack",
    )(wg)


TM = 512


def gelu_tanh(v):
    return v * (0.5 * (1.0 + jnp.tanh(math.sqrt(2.0 / math.pi) * (v + 0.044715 * (v * v * v)))))


def ffn_kernel(tok, act, we, wi, bi, wo, bo, out):
    lane = lax.broadcasted_iota(jnp.int32, (TM, 128), 1)
    col = jnp.transpose(jnp.broadcast_to(tok[0], (128, TM)), (1, 0))
    hot = jnp.concatenate([(col == lane + 128 * j).astype(F32).astype(BF16) for j in range(VOCAB // 128)], axis=1)
    rows = jnp.dot(hot, we[...], preferred_element_type=F32)
    hidden = (rows * math.sqrt(D) + act[...].astype(F32)).astype(BF16)
    step = 512
    total = None
    pre = jnp.dot(hidden, wi[:, 0:step], preferred_element_type=F32)
    for f in range(0, FF, step):
        nxt = None
        if f + step < FF:
            nxt = jnp.dot(hidden, wi[:, f + step:f + 2 * step], preferred_element_type=F32)
        inner = gelu_tanh(pre + bi[:, f:f + step].astype(F32)).astype(BF16)
        part = jnp.dot(inner, wo[f:f + step, :], preferred_element_type=F32)
        total = part if total is None else total + part
        pre = nxt
    out[...] = (total + bo[...].astype(F32)).astype(BF16)


def ffn(tok, act, we, wi, bi, wo, bo):
    tokens = act.shape[0]
    const = lambda i: (0, 0)
    return pl.pallas_call(
        ffn_kernel,
        grid=(tokens // TM,),
        out_shape=jax.ShapeDtypeStruct((tokens, D), BF16),
        in_specs=[
            pl.BlockSpec((1, 1, TM), lambda i: (i, 0, 0)),
            pl.BlockSpec((TM, D), lambda i: (i, 0)),
            pl.BlockSpec((VOCAB, D), const),
            pl.BlockSpec((D, FF), const),
            pl.BlockSpec((1, FF), const),
            pl.BlockSpec((FF, D), const),
            pl.BlockSpec((1, D), const),
        ],
        out_specs=pl.BlockSpec((TM, D), lambda i: (i, 0)),
        compiler_params=pltpu.CompilerParams(vmem_limit_bytes=60_000_000),
        name="ffn",
    )(tok.reshape(tokens // TM, 1, TM), act, we, wi, bi, wo, bo)


def solution(mesh):
    def device_step(g_emb, g_attn, g_in, g_out, g_vecd, g_vecf, opt_m, opt_v, master, tok_ids, act_in):
        gv = jnp.concatenate([g_vecd.reshape(36, 128), g_vecf.reshape(16, 128), jnp.zeros((12, 128), F32)], axis=0)
        m_new, v_new, w_new, wg = comm(
            g_emb.reshape(512, 512), g_attn.reshape(2048, 512), g_in.reshape(512, 2048), g_out.reshape(2048, 512), gv,
            opt_m.reshape(SHARD, 128), opt_v.reshape(SHARD, 128), master.reshape(SHARD, 128))
        we, wa, wi, wo, wv = unpack(wg)
        vecd = wv[:36].reshape(1, 9, 512)
        vecf = wv[36:52].reshape(1, 2048)
        y_out = ffn(tok_ids, act_in, we, wi, vecf, wo, vecd[0, 8:9])
        return (m_new.reshape(-1), v_new.reshape(-1), w_new.reshape(-1), we, wa.reshape(1, 4, 512, 512),
                wi.reshape(1, 512, 2048), wo.reshape(1, 2048, 512), vecd, vecf, y_out)

    grad_specs = tuple(P(AXES, *([None] * (grad_rank - 1))) for grad_rank in GRAD_RANKS)
    in_specs = grad_specs + (P(AXES), P(AXES), P(AXES), P(AXES), P(AXES, None))
    out_specs = (P(AXES), P(AXES), P(AXES), P(), P(), P(), P(), P(), P(), P(AXES, None))
    return jax.shard_map(device_step, mesh=mesh, in_specs=in_specs, out_specs=out_specs, check_vma=False)
```

```python
import functools
import math

import jax
import jax.numpy as jnp
from jax import lax
from jax.experimental import pallas as pl
from jax.experimental.pallas import tpu as pltpu
from jax.sharding import PartitionSpec as P

LEARN_RATE = 0.002
BETA_ONE = 0.9
BETA_TWO = 0.95
ADAM_EPS = 1e-8
ADAM_STEP = 2
AXES = ("dz", "dy", "dx")
GRAD_RANKS = (3, 5, 4, 4, 4, 3)
MESH = pl.DeviceIdType.MESH
F32, BF16 = jnp.float32, jnp.bfloat16

D, FF, VOCAB = 512, 2048, 512
ROWS = 26688
SHARD = 834
WIN = 840
WROWS = 848
TENSORS = ((0, 512, 512), (2048, 2048, 512), (10240, 512, 2048), (18432, 2048, 512))
VEC_ROW = 26624
COLORS = (
    ((3, 2, 1, 0), (0, 136), (0, 144)),
    ((3, 2, 0, 1), (136, 144), (144, 144)),
    ((2, 3, 1, 0), (280, 136), (288, 144)),
    ((2, 3, 0, 1), (416, 144), (432, 144)),
    ((1, 0, 3, 2), (560, 136), (576, 144)),
    ((0, 1, 2, 3), (696, 144), (720, 128)),
)
NC = len(COLORS)


def adam_update(grad_vals, opt_m, opt_v, master):
    m_new = BETA_ONE * opt_m + (1.0 - BETA_ONE) * grad_vals
    v_new = BETA_TWO * opt_v + (1.0 - BETA_TWO) * grad_vals * grad_vals
    m_hat = m_new / (1.0 - BETA_ONE ** ADAM_STEP)
    v_hat = v_new / (1.0 - BETA_TWO ** ADAM_STEP)
    w_new = master - LEARN_RATE * m_hat / (jnp.sqrt(v_hat) + ADAM_EPS)
    return m_new, v_new, w_new


def window_start(s):
    return (s // 4) * 3336 + (s % 4) * 832


def comm_kernel(ge, ga, gi, go, gv, m_in, v_in, w_in, m_out, v_out, w_out, wg_out,
                ne, na, ni, no, flat, acc, r0, r1, r2, r3, r4, ms, vs, ws, wg,
                ld_sem, mvw_sem, s0_s, s0_r, rs_s, rs_r, ag_s, ag_r, pc_s, pc_r, out_sem):
    z, y, xc = lax.axis_index("dz"), lax.axis_index("dy"), lax.axis_index("dx")
    x, c = xc // 2, xc % 2
    b1, b0 = z // 2, z % 2
    g0 = (b0 + b1) % 2
    bits = (b1, g0, y, x)
    peer = (z, y, 2 * x + 1 - c)
    partner = ((3 - z, y, xc), (2 * b1 + 1 - b0, y, xc), (z, 1 - y, xc), (z, y, 2 * (1 - x) + c))

    native = (ne, na, ni, no)
    loads = []
    n_load = 0
    for t, (src, dst, (base, rows, cols)) in enumerate(zip((ge, ga, gi, go), native, TENSORS)):
        chunk = 131072 // cols
        for r in range(0, rows, chunk):
            cp = pltpu.make_async_copy(src.at[pl.ds(r, chunk)], dst.at[pl.ds(r, chunk)], ld_sem.at[n_load])
            cp.start()
            loads.append((cp, t, r, chunk, base + (r + chunk) * cols // 128))
            n_load += 1
    vec_cp = pltpu.make_async_copy(gv, flat.at[pl.ds(VEC_ROW, 64)], ld_sem.at[n_load])
    vec_cp.start()
    mvw = []
    for i, (a, b) in enumerate(((m_in, ms), (v_in, vs), (w_in, ws))):
        cp = pltpu.make_async_copy(a, b, mvw_sem.at[i])
        cp.start()
        mvw.append(cp)

    barrier = pltpu.get_barrier_semaphore()
    for dev in (peer,) + partner:
        pl.semaphore_signal(barrier, inc=1, device_id=dev, device_id_type=MESH)
    pl.semaphore_wait(barrier, 5)

    s0 = []

    def send0(i):
        start = pl.multiple_of(window_start(2 * i + 1 - c), 8)
        cp = pltpu.make_async_remote_copy(flat.at[pl.ds(start, WIN)], r0.at[i], s0_s.at[i], s0_r.at[i],
                                          device_id=peer, device_id_type=MESH)
        cp.start()
        s0.append(cp)

    vec_cp.wait()
    for cp, t, r, chunk, end in loads:
        cp.wait()
        base, _, cols = TENSORS[t]
        lanes = cols // 128

        def group(g, carry, t=t, r=r, base=base, lanes=lanes):
            row = pl.multiple_of(r + g * 8, 8)
            out = base + row * lanes
            for j in range(lanes):
                flat[pl.ds(out + j, 8, stride=lanes), :] = native[t][pl.ds(row, 8), j * 128:(j + 1) * 128]
            return carry

        lax.fori_loop(0, chunk // 8, group, 0, unroll=4 if lanes == 4 else 1)
        if end == VEC_ROW:
            end = ROWS
        while len(s0) < 16 and window_start(2 * len(s0) + 1) + WIN <= end:
            send0(len(s0))

    def slot(i):
        zz = i // 4
        return (zz // 2, (zz % 2 + zz // 2) % 2, (i // 2) % 2, i % 2)

    for i in range(16):
        s0[i].wait_recv()
        start = pl.multiple_of(window_start(2 * i + c), 8)
        acc[slot(i)] = flat[pl.ds(start, WIN), :] + r0[i]

    recv = (r1, r2, r3, r4)
    full = pl.ds(0, 2)

    def rs_copy(k, t):
        order, (row, n), _ = COLORS[k]
        idx = [full] * 4
        for d in order[:t]:
            idx[d] = bits[d]
        idx[order[t]] = 1 - bits[order[t]]
        dst = recv[t].at[(full,) * (3 - t) + (pl.ds(row, n),)]
        return pltpu.make_async_remote_copy(acc.at[tuple(idx) + (pl.ds(row, n),)], dst, rs_s.at[k, t], rs_r.at[k, t],
                                            device_id=partner[order[t]], device_id_type=MESH)

    def rs_add(k, t):
        order, (row, n), _ = COLORS[k]
        idx = [None] * 4
        for d in order[:t + 1]:
            idx[d] = bits[d]
        rest = [d for d in range(4) if idx[d] is None]
        for combo in range(2 ** len(rest)):
            sub = tuple((combo >> (len(rest) - 1 - j)) & 1 for j in range(len(rest)))
            for j, d in enumerate(rest):
                idx[d] = sub[j]
            acc[tuple(idx) + (pl.ds(row, n),)] += recv[t][sub + (pl.ds(row, n),)]

    rs = {}
    for k in range(NC):
        rs[k, 0] = rs_copy(k, 0)
        rs[k, 0].start()
    for t in range(4):
        for k in range(NC):
            rs[k, t].wait_recv()
            rs_add(k, t)
            if t < 3:
                rs[k, t + 1] = rs_copy(k, t + 1)
                rs[k, t + 1].start()

    for cp in mvw:
        cp.wait()
    q = 2 * x + c
    for case in range(4):
        @pl.when(q == case)
        def _():
            grad = acc[bits + (pl.ds(2 * case, SHARD),)] / 32.0
            m_new, v_new, w_new = adam_update(grad, ms[...], vs[...], ws[...])
            ms[...] = m_new
            vs[...] = v_new
            ws[...] = w_new
            wg[(c,) + bits + (pl.ds(SHARD - 2, 16),)] = jnp.zeros((16, 128), BF16)
            wg[(c,) + bits + (pl.ds(0, SHARD),)] = w_new.astype(BF16)
    outs = []
    for i, (a, b) in enumerate(((ms, m_out), (vs, v_out), (ws, w_out))):
        cp = pltpu.make_async_copy(a, b, out_sem.at[i])
        cp.start()
        outs.append(cp)

    def ag_idx(k, t, mine):
        order = COLORS[k][0]
        idx = [full] * 4
        for d in order[:t]:
            idx[d] = bits[d]
        if t < 4:
            idx[order[t]] = bits[order[t]] if mine else 1 - bits[order[t]]
        return (c,) + tuple(idx) + (pl.ds(*COLORS[k][2]),)

    def ag_copy(k, t):
        ref = wg.at[ag_idx(k, t, True)]
        return pltpu.make_async_remote_copy(ref, ref, ag_s.at[k, t], ag_r.at[k, t],
                                            device_id=partner[COLORS[k][0][t]], device_id_type=MESH)

    def pc_copy(k, t):
        ref = wg.at[ag_idx(k, t, False) if t < 4 else (c,) + bits + (pl.ds(*COLORS[k][2]),)]
        return pltpu.make_async_remote_copy(ref, ref, pc_s.at[k, t], pc_r.at[k, t],
                                            device_id=peer, device_id_type=MESH)

    ag, pc = {}, {}
    for k in range(NC):
        ag[k, 3] = ag_copy(k, 3)
        ag[k, 3].start()
    for k in range(NC):
        pc[k, 4] = pc_copy(k, 4)
        pc[k, 4].start()
    for t in (3, 2, 1, 0):
        for k in range(NC):
            ag[k, t].wait_recv()
            if t > 0:
                ag[k, t - 1] = ag_copy(k, t - 1)
                ag[k, t - 1].start()
            pc[k, t] = pc_copy(k, t)
            pc[k, t].start()
    for t in (4, 3, 2, 1, 0):
        for k in range(NC):
            pc[k, t].wait_recv()
    cp = pltpu.make_async_copy(wg, wg_out, out_sem.at[3])
    cp.start()
    outs.append(cp)
    for cp in s0 + list(rs.values()) + list(ag.values()) + list(pc.values()):
        cp.wait_send()
    for cp in outs:
        cp.wait()


def comm(ge, ga, gi, go, gv, m, v, w):
    any_spec = pl.BlockSpec(memory_space=pl.ANY)
    shard = jax.ShapeDtypeStruct((SHARD, 128), F32)
    dma = pltpu.SemaphoreType.DMA
    return pl.pallas_call(
        comm_kernel,
        out_shape=(shard, shard, shard, jax.ShapeDtypeStruct((2, 2, 2, 2, 2, WROWS, 128), BF16)),
        in_specs=[any_spec] * 8,
        out_specs=(any_spec,) * 4,
        scratch_shapes=[
            pltpu.VMEM((512, 512), F32), pltpu.VMEM((2048, 512), F32),
            pltpu.VMEM((512, 2048), F32), pltpu.VMEM((2048, 512), F32),
            pltpu.VMEM((ROWS, 128), F32),
            pltpu.VMEM((2, 2, 2, 2, WIN, 128), F32),
            pltpu.VMEM((16, WIN, 128), F32),
            pltpu.VMEM((2, 2, 2, WIN, 128), F32), pltpu.VMEM((2, 2, WIN, 128), F32),
            pltpu.VMEM((2, WIN, 128), F32), pltpu.VMEM((WIN, 128), F32),
            pltpu.VMEM((SHARD, 128), F32), pltpu.VMEM((SHARD, 128), F32), pltpu.VMEM((SHARD, 128), F32),
            pltpu.VMEM((2, 2, 2, 2, 2, WROWS, 128), BF16),
            dma((32,)), dma((3,)), dma((16,)), dma((16,)),
            dma((NC, 4)), dma((NC, 4)), dma((NC, 4)), dma((NC, 4)), dma((NC, 5)), dma((NC, 5)), dma((4,)),
        ],
        compiler_params=pltpu.CompilerParams(collective_id=0, has_side_effects=True, vmem_limit_bytes=66_000_000),
        name="comm",
    )(ge, ga, gi, go, gv, m, v, w)


def unpack_kernel(wg, we, wa, wi, wo, wv, flat):
    for s in range(32):
        i, core = s // 2, s % 2
        zz = i // 4
        idx = (core, zz // 2, (zz % 2 + zz // 2) % 2, (i // 2) % 2, i % 2)
        flat[pl.ds(s * SHARD, SHARD), :] = wg[idx + (pl.ds(0, SHARD),)].astype(F32)
    for dst, (base, rows, cols) in zip((we, wa, wi, wo), TENSORS):
        lanes = cols // 128

        def group(g, carry, dst=dst, base=base, lanes=lanes):
            row = pl.multiple_of(g * 16, 16)
            for j in range(lanes):
                dst[pl.ds(row, 16), j * 128:(j + 1) * 128] = flat[
                    pl.ds(base + row * lanes + j, 16, stride=lanes), :].astype(BF16)
            return carry

        lax.fori_loop(0, rows // 16, group, 0, unroll=4 if lanes == 4 else 1)
    wv[...] = flat[pl.ds(VEC_ROW, 64), :].astype(BF16)


def unpack(wg):
    vm = pl.BlockSpec(memory_space=pltpu.VMEM)
    shapes = [(512, 512), (2048, 512), (512, 2048), (2048, 512), (64, 128)]
    return pl.pallas_call(
        unpack_kernel,
        out_shape=tuple(jax.ShapeDtypeStruct(s, BF16) for s in shapes),
        in_specs=[vm],
        out_specs=(vm,) * 5,
        scratch_shapes=[pltpu.VMEM((ROWS, 128), F32)],
        compiler_params=pltpu.CompilerParams(vmem_limit_bytes=60_000_000),
        name="unpack",
    )(wg)


TM = 1024


def gelu_tanh(v):
    c = math.sqrt(2.0 / math.pi)
    half = 0.5 * v
    return half + half * jnp.tanh(v * (c + (c * 0.044715) * (v * v)))


def ffn_kernel(tok, act, we, wi, bi, wo, bo, out):
    lane = lax.broadcasted_iota(jnp.int32, (TM, 128), 1)
    col = jnp.transpose(jnp.broadcast_to(tok[0], (128, TM)), (1, 0))
    hot = jnp.concatenate([(col == lane + 128 * j).astype(F32).astype(BF16) for j in range(VOCAB // 128)], axis=1)
    rows = jnp.dot(hot, we[...], preferred_element_type=F32)
    hidden = (rows * math.sqrt(D) + act[...].astype(F32)).astype(BF16)
    step = 512
    parts = []
    pre = jnp.dot(hidden, wi[:, 0:step], preferred_element_type=F32)
    for f in range(0, FF, step):
        nxt = None
        if f + step < FF:
            nxt = jnp.dot(hidden, wi[:, f + step:f + 2 * step], preferred_element_type=F32)
        parts.append(gelu_tanh(pre + bi[:, f:f + step].astype(F32)).astype(BF16))
        pre = nxt
    inner = jnp.concatenate(parts, axis=1)
    total = jnp.dot(inner, wo[...], preferred_element_type=F32)
    out[...] = (total + bo[...].astype(F32)).astype(BF16)


def ffn(tok, act, we, wi, bi, wo, bo):
    tokens = act.shape[0]
    const = lambda i: (0, 0)
    return pl.pallas_call(
        ffn_kernel,
        grid=(tokens // TM,),
        out_shape=jax.ShapeDtypeStruct((tokens, D), BF16),
        in_specs=[
            pl.BlockSpec((1, 1, TM), lambda i: (i, 0, 0)),
            pl.BlockSpec((TM, D), lambda i: (i, 0)),
            pl.BlockSpec((VOCAB, D), const),
            pl.BlockSpec((D, FF), const),
            pl.BlockSpec((1, FF), const),
            pl.BlockSpec((FF, D), const),
            pl.BlockSpec((1, D), const),
        ],
        out_specs=pl.BlockSpec((TM, D), lambda i: (i, 0)),
        compiler_params=pltpu.CompilerParams(vmem_limit_bytes=60_000_000),
        name="ffn",
    )(tok.reshape(tokens // TM, 1, TM), act, we, wi, bi, wo, bo)


def solution(mesh):
    def device_step(g_emb, g_attn, g_in, g_out, g_vecd, g_vecf, opt_m, opt_v, master, tok_ids, act_in):
        gv = jnp.concatenate([g_vecd.reshape(36, 128), g_vecf.reshape(16, 128), jnp.zeros((12, 128), F32)], axis=0)
        m_new, v_new, w_new, wg = comm(
            g_emb.reshape(512, 512), g_attn.reshape(2048, 512), g_in.reshape(512, 2048), g_out.reshape(2048, 512), gv,
            opt_m.reshape(SHARD, 128), opt_v.reshape(SHARD, 128), master.reshape(SHARD, 128))
        we, wa, wi, wo, wv = unpack(wg)
        vecd = wv[:36].reshape(1, 9, 512)
        vecf = wv[36:52].reshape(1, 2048)
        y_out = ffn(tok_ids, act_in, we, wi, vecf, wo, vecd[0, 8:9])
        return (m_new.reshape(-1), v_new.reshape(-1), w_new.reshape(-1), we, wa.reshape(1, 4, 512, 512),
                wi.reshape(1, 512, 2048), wo.reshape(1, 2048, 512), vecd, vecf, y_out)

    grad_specs = tuple(P(AXES, *([None] * (grad_rank - 1))) for grad_rank in GRAD_RANKS)
    in_specs = grad_specs + (P(AXES), P(AXES), P(AXES), P(AXES), P(AXES, None))
    out_specs = (P(AXES), P(AXES), P(AXES), P(), P(), P(), P(), P(), P(), P(AXES, None))
    return jax.shard_map(device_step, mesh=mesh, in_specs=in_specs, out_specs=out_specs, check_vma=False)
```

```python
import functools
import math

import jax
import jax.numpy as jnp
from jax import lax
from jax.experimental import pallas as pl
from jax.experimental.pallas import tpu as pltpu
from jax.sharding import PartitionSpec as P

LEARN_RATE = 0.002
BETA_ONE = 0.9
BETA_TWO = 0.95
ADAM_EPS = 1e-8
ADAM_STEP = 2
AXES = ("dz", "dy", "dx")
GRAD_RANKS = (3, 5, 4, 4, 4, 3)
MESH = pl.DeviceIdType.MESH
F32, BF16 = jnp.float32, jnp.bfloat16

D, FF, VOCAB, LN = 512, 2048, 512, 128
ROWS = 26688
SHARD = 834
WIN = 840
WROWS = 848
TENSORS = ((0, 512, 512), (2048, 2048, 512), (10240, 512, 2048), (18432, 2048, 512))
VEC_ROW = 26624
X, Y, ZA, ZB = 3, 2, 1, 0
BACK = (3, 2, 1, 0)
ORDERS = ((X, Y, ZA, ZB), (X, Y, ZB, ZA), (Y, X, ZA, ZB), (Y, X, ZB, ZA), (ZA, ZB, X, Y), (ZB, ZA, Y, X))
RS_ROWS = (72, 64, 72, 64, 72, 72, 72, 72, 72, 72, 64, 72)
AG_ROWS = (80, 64, 80, 64, 64, 64, 80, 64, 80, 64, 64, 80)
NC = len(RS_ROWS)
COLORS = tuple((ORDERS[k % len(ORDERS)], (sum(RS_ROWS[:k]), RS_ROWS[k]), (sum(AG_ROWS[:k]), AG_ROWS[k]))
               for k in range(NC))
GROUPS = ((0, sum(RS_ROWS[:6])), (sum(RS_ROWS[:6]), sum(RS_ROWS[6:])))
CHUNK, CHUNK_ROWS = 131072, 1024
RING = 6, 4


def window_start(s):
    return (s // 4) * 3336 + (s % 4) * 832


def adam_update(grad_vals, opt_m, opt_v, master):
    m_new = BETA_ONE * opt_m + (1.0 - BETA_ONE) * grad_vals
    v_new = BETA_TWO * opt_v + (1.0 - BETA_TWO) * grad_vals * grad_vals
    m_hat = m_new / (1.0 - BETA_ONE ** ADAM_STEP)
    v_hat = v_new / (1.0 - BETA_TWO ** ADAM_STEP)
    w_new = master - LEARN_RATE * m_hat / (jnp.sqrt(v_hat) + ADAM_EPS)
    return m_new, v_new, w_new


def window_start(s):
    return (s // 4) * 3336 + (s % 4) * 832


def gelu_tanh(v):
    c = math.sqrt(2.0 / math.pi)
    half = 0.5 * v
    return half + half * jnp.tanh(v * (c + (c * 0.044715) * (v * v)))


def spread(wg, flat, shards):
    for s in shards:
        idx = (s % 2,) + slot(s // 2)
        flat[pl.ds(s * SHARD, SHARD), :] = wg[idx + (pl.ds(0, SHARD),)].astype(F32)


def to_native(flat, dst, tensor, unroll):
    base, rows, cols = TENSORS[tensor]
    lanes = cols // LN

    def group(g, carry):
        row = pl.multiple_of(g * 16, 16)
        for j in range(lanes):
            dst[pl.ds(row, 16), j * LN:(j + 1) * LN] = flat[
                pl.ds(base + row * lanes + j, 16, stride=lanes), :].astype(BF16)
        return carry

    lax.fori_loop(0, rows // 16, group, 0, unroll=unroll)


def slot(i):
    z = i // 4
    return (z // 2, (z % 2 + z // 2) % 2, (i // 2) % 2, i % 2)


def comm_kernel(ge, ga, gi, go, gvd, gvf, m_in, v_in, w_in, m_out, v_out, w_out, we_out, wa_out, wi_out, wo_out,
                wvd_out, wvf_out,
                st5, st20, svd, svf, flat, acc, r1, r2, r3, r4, gs, ms, vs, ws, mo, vo, wn, wg, we, wa, wi, wo, wvd, wvf,
                ld_sem, mvw_sem, s0_s, s0_r, rs_s, rs_r, ag_s, ag_r, pc_s, pc_r, out_sem):
    z, y, xc = lax.axis_index("dz"), lax.axis_index("dy"), lax.axis_index("dx")
    x, c = xc // 2, xc % 2
    b1, b0 = z // 2, z % 2
    g0 = (b0 + b1) % 2
    bits = (b1, g0, y, x)
    peer = (z, y, 2 * x + 1 - c)
    partner = ((3 - z, y, xc), (2 * b1 + 1 - b0, y, xc), (z, 1 - y, xc), (z, y, 2 * (1 - x) + c))

    srcs = (ge, ga, gi, go)
    order = [(t, j) for t, (_, rows, cols) in enumerate(TENSORS) for j in range(rows * cols // CHUNK)]
    seq = ([ch for ch in order if ch[0] != 2], [ch for ch in order if ch[0] == 2])
    ring_of = (st5, st20)

    def load(kind, pos):
        t, j = seq[kind][pos]
        rows = CHUNK // TENSORS[t][2]
        at = pos % RING[kind]
        return pltpu.make_async_copy(srcs[t].at[pl.ds(j * rows, rows)], ring_of[kind].at[at],
                                     ld_sem.at[kind * RING[0] + at])

    for kind in range(2):
        for pos in range(RING[kind]):
            load(kind, pos).start()
    vec = [pltpu.make_async_copy(a, b, ld_sem.at[sum(RING) + i]) for i, (a, b) in enumerate(((gvd, svd), (gvf, svf)))]
    mvw = [pltpu.make_async_copy(a, b, mvw_sem.at[i]) for i, (a, b) in enumerate(((m_in, ms), (v_in, vs), (w_in, ws)))]
    for cp in vec + mvw:
        cp.start()

    barrier = pltpu.get_barrier_semaphore()
    for dev in (peer,) + partner:
        pl.semaphore_signal(barrier, inc=1, device_id=dev, device_id_type=MESH)
    pl.semaphore_wait(barrier, 5)

    done = [0, 0]

    def take(ch):
        t, j = ch
        kind = 1 if t == 2 else 0
        pos = done[kind]
        assert seq[kind][pos] == ch
        load(kind, pos).wait()
        base, _, cols = TENSORS[t]
        lanes = cols // LN
        rows = CHUNK // cols
        slot = pos % RING[kind]
        ring = ring_of[kind]

        def group(g, carry):
            row = pl.multiple_of(g * 8, 8)
            out = base + (j * rows + row) * lanes
            for i in range(lanes):
                flat[pl.ds(out + i, 8, stride=lanes), :] = ring[slot, pl.ds(row, 8), i * LN:(i + 1) * LN]
            return carry

        lax.fori_loop(0, rows // 8, group, 0, unroll=4 if lanes == 4 else 1)
        done[kind] += 1
        if pos + RING[kind] < len(seq[kind]):
            load(kind, pos + RING[kind]).start()

    def s0_copy(i, g):
        row, n = GROUPS[g]
        start = pl.multiple_of(window_start(2 * i + 1 - c) + row, 8)
        return pltpu.make_async_remote_copy(flat.at[pl.ds(start, n)], acc.at[slot(i) + (pl.ds(row, n),)],
                                            s0_s.at[g, i], s0_r.at[g, i], device_id=peer, device_id_type=MESH)

    def s0_add(i, g):
        row, n = GROUPS[g]
        s0_copy(i, g).wait_recv()
        start = pl.multiple_of(window_start(2 * i + c) + row, 8)
        acc[slot(i) + (pl.ds(row, n),)] += flat[pl.ds(start, n), :]

    sent = 0
    for ch in order:
        take(ch)
        end = TENSORS[ch[0]][0] + (ch[1] + 1) * CHUNK_ROWS
        if end == VEC_ROW:
            for cp in vec:
                cp.wait()
            for j in range(4):
                flat[pl.ds(VEC_ROW + j, 9, stride=4), :] = svd[:, j * LN:(j + 1) * LN]
            for j in range(16):
                flat[pl.ds(VEC_ROW + 36 + j, 1), :] = svf[:, j * LN:(j + 1) * LN]
            flat[pl.ds(VEC_ROW + 52, 12), :] = jnp.zeros((12, LN), F32)
            end = ROWS
        while sent < 16 and window_start(2 * sent + 1) + WIN <= end:
            s0_copy(sent, 0).start()
            sent += 1
            if sent > 1:
                s0_add(sent - 2, 0)
    s0_add(15, 0)
    for i in range(16):
        s0_copy(i, 1).start()

    recv = (r1, r2, r3, r4)
    both = pl.ds(0, 2)

    def rs_copy(k, t):
        o, (row, n), _ = COLORS[k]
        idx = [both] * 4
        for d in o[:t]:
            idx[d] = bits[d]
        idx[o[t]] = 1 - bits[o[t]]
        dst = recv[t].at[(both,) * (3 - t) + (pl.ds(row, n),)]
        return pltpu.make_async_remote_copy(acc.at[tuple(idx) + (pl.ds(row, n),)], dst, rs_s.at[k, t], rs_r.at[k, t],
                                            device_id=partner[o[t]], device_id_type=MESH)

    def rs_add(k, t):
        o, (row, n), _ = COLORS[k]
        idx = [None] * 4
        for d in o[:t + 1]:
            idx[d] = bits[d]
        rest = [d for d in range(4) if d not in o[:t + 1]]
        for combo in range(2 ** len(rest)):
            sub = tuple((combo >> (len(rest) - 1 - j)) & 1 for j in range(len(rest)))
            for j, d in enumerate(rest):
                idx[d] = sub[j]
            acc[tuple(idx) + (pl.ds(row, n),)] += recv[t][sub + (pl.ds(row, n),)]

    rs = {}

    def rs_start(k, t):
        rs[k, t] = rs_copy(k, t)
        rs[k, t].start()

    for k in range(6):
        rs_start(k, 0)
    for i in range(16):
        s0_add(i, 1)
    for k in range(6, NC):
        rs_start(k, 0)
    for t in range(4):
        for k in range(NC):
            rs[k, t].wait_recv()
            rs_add(k, t)
            if t < 3:
                rs_start(k, t + 1)

    for cp in mvw:
        cp.wait()
    q = 2 * x + c
    for case in range(4):
        @pl.when(q == case)
        def _():
            gs[...] = acc[bits + (pl.ds(2 * case, SHARD),)]

    def rows(sl):
        m_new, v_new, w_new = adam_update(gs[sl, :] / 32.0, ms[sl, :], vs[sl, :], ws[sl, :])
        mo[sl, :] = m_new
        vo[sl, :] = v_new
        wn[sl, :] = w_new
        wg[(c,) + bits + (sl,)] = w_new.astype(BF16)

    def block(i, carry):
        rows(pl.ds(pl.multiple_of(i * 16, 16), 16))
        return carry

    lax.fori_loop(0, 52, block, 0, unroll=4)
    wg[(c,) + bits + (pl.ds(832, 16),)] = jnp.zeros((16, LN), BF16)
    rows(pl.ds(832, 2))
    outs = []

    def put(pairs):
        for a, b in pairs:
            cp = pltpu.make_async_copy(a, b, out_sem.at[len(outs)])
            cp.start()
            outs.append(cp)

    def ag_idx(k, t, kept):
        o = COLORS[k][0]
        idx = [both] * 4
        for d in o[:t]:
            idx[d] = bits[d]
        if t < 4:
            idx[o[t]] = bits[o[t]] if kept else 1 - bits[o[t]]
        return (c,) + tuple(idx) + (pl.ds(*COLORS[k][2]),)

    def ag_copy(k, t):
        ref = wg.at[ag_idx(k, t, True)]
        return pltpu.make_async_remote_copy(ref, ref, ag_s.at[k, t], ag_r.at[k, t],
                                            device_id=partner[COLORS[k][0][t]], device_id_type=MESH)

    def pc_copy(k, t):
        ref = wg.at[ag_idx(k, t, False)]
        return pltpu.make_async_remote_copy(ref, ref, pc_s.at[k, t], pc_r.at[k, t],
                                            device_id=peer, device_id_type=MESH)

    ag, pc = {}, {}

    def ag_start(k, t):
        ag[k, t] = ag_copy(k, t)
        ag[k, t].start()

    def pc_start(k, t):
        pc[k, t] = pc_copy(k, t)
        pc[k, t].start()

    for k in range(NC):
        ag_start(k, 3)
    for k in range(NC):
        pc_start(k, 4)
    put(((mo, m_out), (vo, v_out), (wn, w_out)))
    for t in BACK:
        for k in range(NC):
            ag[k, t].wait_recv()
            if t > 0:
                ag_start(k, t - 1)
            pc_start(k, t)
    for cp in [rs[key] for key in rs]:
        cp.wait_send()
    for g in range(2):
        for i in range(16):
            s0_copy(i, g).wait_send()
    for t in BACK:
        for k in range(NC):
            pc[k, t].wait_recv()
    for k in range(NC):
        pc[k, 4].wait_recv()

    spread(wg, flat, range(32))
    for i, (ref, out) in enumerate(((we, we_out), (wi, wi_out), (wo, wo_out), (wa, wa_out))):
        to_native(flat, ref, (0, 2, 3, 1)[i], 1 if ref is wi else 4)
        put(((ref, out),))
    for j in range(4):
        wvd[:, j * LN:(j + 1) * LN] = flat[pl.ds(VEC_ROW + j, 9, stride=4), :].astype(BF16)
    for j in range(16):
        wvf[:, j * LN:(j + 1) * LN] = flat[pl.ds(VEC_ROW + 36 + j, 1), :].astype(BF16)
    put(((wvd, wvd_out), (wvf, wvf_out)))
    for cp in list(ag.values()) + list(pc.values()):
        cp.wait_send()
    for cp in outs:
        cp.wait()


def comm(*args):
    hbm = pl.BlockSpec(memory_space=pl.ANY)
    shard = jax.ShapeDtypeStruct((SHARD, LN), F32)
    dma = pltpu.SemaphoreType.DMA
    weights = ((VOCAB, D), (FF, D), (D, FF), (FF, D), (9, D), (1, FF))
    return pl.pallas_call(
        comm_kernel,
        out_shape=(shard,) * 3 + tuple(jax.ShapeDtypeStruct(s, BF16) for s in weights),
        in_specs=[hbm] * 9,
        out_specs=(hbm,) * 9,
        scratch_shapes=[
            pltpu.VMEM((RING[0], CHUNK // D, D), F32), pltpu.VMEM((RING[1], CHUNK // FF, FF), F32),
            pltpu.VMEM((9, D), F32), pltpu.VMEM((1, FF), F32),
            pltpu.VMEM((ROWS, LN), F32)]
        + [pltpu.VMEM((2,) * n + (WIN, LN), F32) for n in (4,) + BACK]
        + [pltpu.VMEM((SHARD, LN), F32)] * 7
        + [pltpu.VMEM((2,) * 5 + (WROWS, LN), BF16)]
        + [pltpu.VMEM(s, BF16) for s in weights]
        + [dma((sum(RING) + 2,)), dma((3,)), dma((2, 16)), dma((2, 16))]
        + [dma((NC, 4))] * 4 + [dma((NC, 5))] * 2 + [dma((9,))],
        compiler_params=pltpu.CompilerParams(collective_id=0, has_side_effects=True, vmem_limit_bytes=66_000_000),
        name="comm",
    )(*args)


TM = 1024


def ffn_kernel(tok, act, we, wa, wi, wo, wvd, wvf, m_in, v_in, w_in,
               out, we_out, wa_out, wi_out, wo_out, wvd_out, wvf_out, m_out, v_out, w_out):
    i = pl.program_id(0)

    @pl.when(i == 0)
    def _():
        for a, b in ((wvd, wvd_out), (wvf, wvf_out), (m_in, m_out), (v_in, v_out), (w_in, w_out)):
            b[...] = a[...]

    wa_out[...] = wa[...]
    for a, b in ((we, we_out), (wi, wi_out), (wo, wo_out)):
        n = b.shape[0]
        b[...] = a[pl.ds(pl.multiple_of(i * n, n), n), :]
    lane = lax.broadcasted_iota(jnp.int32, (TM, LN), 1)
    col = jnp.transpose(jnp.broadcast_to(tok[0], (LN, TM)), (1, 0))
    hot = jnp.concatenate([(col == lane + LN * j).astype(F32).astype(BF16) for j in range(VOCAB // LN)], axis=1)
    rows = jnp.dot(hot, we[...], preferred_element_type=F32)
    hidden = (rows * math.sqrt(D) + act[...].astype(F32)).astype(BF16)
    step = 512
    parts = []
    pre = jnp.dot(hidden, wi[:, 0:step], preferred_element_type=F32)
    for f in range(0, FF, step):
        nxt = None
        if f + step < FF:
            nxt = jnp.dot(hidden, wi[:, f + step:f + 2 * step], preferred_element_type=F32)
        parts.append(gelu_tanh(pre + wvf[:, f:f + step].astype(F32)).astype(BF16))
        pre = nxt
    inner = jnp.concatenate(parts, axis=1)
    total = jnp.dot(inner, wo[...], preferred_element_type=F32)
    out[...] = (total + wvd[8:9, :].astype(F32)).astype(BF16)


def ffn(tok, act, *rest):
    tokens = act.shape[0]
    steps = tokens // TM
    row = lambda i: (i, 0)

    def whole(ref):
        return pl.BlockSpec(ref.shape, lambda i: (0, 0))

    def part(ref):
        return pl.BlockSpec((ref.shape[0] // steps, ref.shape[1]), row)

    we, wa, wi, wo, wvd, wvf, m, v, w = rest
    outs = (we, wa, wi, wo, wvd, wvf, m, v, w)
    return pl.pallas_call(
        ffn_kernel,
        grid=(steps,),
        out_shape=(jax.ShapeDtypeStruct(act.shape, BF16),) + tuple(jax.ShapeDtypeStruct(a.shape, a.dtype) for a in outs),
        in_specs=[pl.BlockSpec((1, 1, TM), lambda i: (i, 0, 0)), part(act), whole(we), part(wa), whole(wi), whole(wo)]
        + [whole(a) for a in (wvd, wvf, m, v, w)],
        out_specs=(part(act), part(we), part(wa), part(wi), part(wo)) + tuple(whole(a) for a in (wvd, wvf, m, v, w)),
        compiler_params=pltpu.CompilerParams(vmem_limit_bytes=66_000_000),
        name="ffn",
    )(tok.reshape(steps, 1, TM), act, *rest)


def solution(mesh):
    def device_step(g_emb, g_attn, g_in, g_out, g_vecd, g_vecf, opt_m, opt_v, master, tok_ids, act_in):
        m1, v1, w1, *weights = comm(
            g_emb.reshape(VOCAB, D), g_attn.reshape(FF, D), g_in.reshape(D, FF), g_out.reshape(FF, D),
            g_vecd.reshape(9, D), g_vecf.reshape(1, FF),
            opt_m.reshape(SHARD, LN), opt_v.reshape(SHARD, LN), master.reshape(SHARD, LN))
        y_out, we, wa, wi, wo, wvd, wvf, m_new, v_new, w_new = ffn(tok_ids, act_in, *weights, m1, v1, w1)
        return (m_new.reshape(-1), v_new.reshape(-1), w_new.reshape(-1), we, wa.reshape(1, 4, D, D),
                wi.reshape(1, D, FF), wo.reshape(1, FF, D), wvd.reshape(1, 9, D), wvf, y_out)

    grad_specs = tuple(P(AXES, *([None] * (grad_rank - 1))) for grad_rank in GRAD_RANKS)
    in_specs = grad_specs + (P(AXES), P(AXES), P(AXES), P(AXES), P(AXES, None))
    out_specs = (P(AXES), P(AXES), P(AXES), P(), P(), P(), P(), P(), P(), P(AXES, None))
    return jax.shard_map(device_step, mesh=mesh, in_specs=in_specs, out_specs=out_specs, check_vma=False)
```

```python
import functools
import math

import jax
import jax.numpy as jnp
from jax import lax
from jax.experimental import pallas as pl
from jax.experimental.pallas import tpu as pltpu
from jax.sharding import PartitionSpec as P

LEARN_RATE = 0.002
BETA_ONE = 0.9
BETA_TWO = 0.95
ADAM_EPS = 1e-8
ADAM_STEP = 2
AXES = ("dz", "dy", "dx")
GRAD_RANKS = (3, 5, 4, 4, 4, 3)
MESH = pl.DeviceIdType.MESH
F32, BF16 = jnp.float32, jnp.bfloat16

D, FF, VOCAB, LN = 512, 2048, 512, 128
ROWS = 26688
SHARD = 834
WIN = 840
WROWS = 848
TENSORS = ((0, 512, 512), (2048, 2048, 512), (10240, 512, 2048), (18432, 2048, 512))
VEC_ROW = 26624
X, Y, ZA, ZB = 3, 2, 1, 0
BACK = (3, 2, 1, 0)
ORDERS = ((X, Y, ZA, ZB), (X, Y, ZB, ZA), (Y, X, ZA, ZB), (Y, X, ZB, ZA), (ZA, ZB, X, Y), (ZB, ZA, Y, X))
RS_ROWS = (72, 64, 72, 64, 72, 72, 72, 72, 72, 72, 64, 72)
AG_ROWS = (64, 64, 64, 64, 64, 80, 80, 64, 80, 80, 64, 80)
NC = len(RS_ROWS)
COLORS = tuple((ORDERS[k % len(ORDERS)], (sum(RS_ROWS[:k]), RS_ROWS[k]), (sum(AG_ROWS[:k]), AG_ROWS[k]))
               for k in range(NC))
EARLY_ROWS = sum(AG_ROWS[:6])
GROUPS = ((0, sum(RS_ROWS[:6])), (sum(RS_ROWS[:6]), sum(RS_ROWS[6:])))
CHUNK, CHUNK_ROWS = 131072, 1024
RING = 6, 4


def window_start(s):
    return (s // 4) * 3336 + (s % 4) * 832


def adam_update(grad_vals, opt_m, opt_v, master):
    m_new = BETA_ONE * opt_m + (1.0 - BETA_ONE) * grad_vals
    v_new = BETA_TWO * opt_v + (1.0 - BETA_TWO) * grad_vals * grad_vals
    m_hat = m_new / (1.0 - BETA_ONE ** ADAM_STEP)
    v_hat = v_new / (1.0 - BETA_TWO ** ADAM_STEP)
    w_new = master - LEARN_RATE * m_hat / (jnp.sqrt(v_hat) + ADAM_EPS)
    return m_new, v_new, w_new


def window_start(s):
    return (s // 4) * 3336 + (s % 4) * 832


def gelu_tanh(v):
    c = math.sqrt(2.0 / math.pi)
    half = 0.5 * v
    return half + half * jnp.tanh(v * (c + (c * 0.044715) * (v * v)))


def spread(wg, flat, row, n):
    for s in range(32):
        idx = (s % 2,) + slot(s // 2)
        flat[pl.ds(s * SHARD + row, n), :] = wg[idx + (pl.ds(row, n),)].astype(F32)


def to_native(flat, dst, tensor, unroll):
    base, rows, cols = TENSORS[tensor]
    lanes = cols // LN

    def group(g, carry):
        row = pl.multiple_of(g * 16, 16)
        for j in range(lanes):
            dst[pl.ds(row, 16), j * LN:(j + 1) * LN] = flat[
                pl.ds(base + row * lanes + j, 16, stride=lanes), :].astype(BF16)
        return carry

    lax.fori_loop(0, rows // 16, group, 0, unroll=unroll)


def slot(i):
    z = i // 4
    return (z // 2, (z % 2 + z // 2) % 2, (i // 2) % 2, i % 2)


def comm_kernel(ge, ga, gi, go, gvd, gvf, m_in, v_in, w_in, m_out, v_out, w_out, we_out, wa_out, wi_out, wo_out,
                wvd_out, wvf_out,
                st5, st20, svd, svf, flat, acc, r1, r2, r3, r4, gs, ms, vs, ws, mo, vo, wn, wg, we, wa, wi, wo, wvd, wvf,
                ld_sem, mvw_sem, s0_s, s0_r, rs_s, rs_r, ag_s, ag_r, pc_s, pc_r, out_sem):
    z, y, xc = lax.axis_index("dz"), lax.axis_index("dy"), lax.axis_index("dx")
    x, c = xc // 2, xc % 2
    b1, b0 = z // 2, z % 2
    g0 = (b0 + b1) % 2
    bits = (b1, g0, y, x)
    peer = (z, y, 2 * x + 1 - c)
    partner = ((3 - z, y, xc), (2 * b1 + 1 - b0, y, xc), (z, 1 - y, xc), (z, y, 2 * (1 - x) + c))

    srcs = (ge, ga, gi, go)
    order = [(t, j) for t, (_, rows, cols) in enumerate(TENSORS) for j in range(rows * cols // CHUNK)]
    seq = ([ch for ch in order if ch[0] != 2], [ch for ch in order if ch[0] == 2])
    ring_of = (st5, st20)

    def load(kind, pos):
        t, j = seq[kind][pos]
        rows = CHUNK // TENSORS[t][2]
        at = pos % RING[kind]
        return pltpu.make_async_copy(srcs[t].at[pl.ds(j * rows, rows)], ring_of[kind].at[at],
                                     ld_sem.at[kind * RING[0] + at])

    for kind in range(2):
        for pos in range(RING[kind]):
            load(kind, pos).start()
    vec = [pltpu.make_async_copy(a, b, ld_sem.at[sum(RING) + i]) for i, (a, b) in enumerate(((gvd, svd), (gvf, svf)))]
    mvw = [pltpu.make_async_copy(a, b, mvw_sem.at[i]) for i, (a, b) in enumerate(((m_in, ms), (v_in, vs), (w_in, ws)))]
    for cp in vec + mvw:
        cp.start()

    barrier = pltpu.get_barrier_semaphore()
    for dev in (peer,) + partner:
        pl.semaphore_signal(barrier, inc=1, device_id=dev, device_id_type=MESH)
    pl.semaphore_wait(barrier, 5)

    done = [0, 0]

    def take(ch):
        t, j = ch
        kind = 1 if t == 2 else 0
        pos = done[kind]
        assert seq[kind][pos] == ch
        load(kind, pos).wait()
        base, _, cols = TENSORS[t]
        lanes = cols // LN
        rows = CHUNK // cols
        slot = pos % RING[kind]
        ring = ring_of[kind]

        def group(g, carry):
            row = pl.multiple_of(g * 8, 8)
            out = base + (j * rows + row) * lanes
            for i in range(lanes):
                flat[pl.ds(out + i, 8, stride=lanes), :] = ring[slot, pl.ds(row, 8), i * LN:(i + 1) * LN]
            return carry

        lax.fori_loop(0, rows // 8, group, 0, unroll=4 if lanes == 4 else 1)
        done[kind] += 1
        if pos + RING[kind] < len(seq[kind]):
            load(kind, pos + RING[kind]).start()

    def s0_copy(i, g):
        row, n = GROUPS[g]
        start = pl.multiple_of(window_start(2 * i + 1 - c) + row, 8)
        return pltpu.make_async_remote_copy(flat.at[pl.ds(start, n)], acc.at[slot(i) + (pl.ds(row, n),)],
                                            s0_s.at[g, i], s0_r.at[g, i], device_id=peer, device_id_type=MESH)

    def s0_add(i, g):
        row, n = GROUPS[g]
        s0_copy(i, g).wait_recv()
        start = pl.multiple_of(window_start(2 * i + c) + row, 8)
        acc[slot(i) + (pl.ds(row, n),)] += flat[pl.ds(start, n), :]

    sent = 0
    for ch in order:
        take(ch)
        end = TENSORS[ch[0]][0] + (ch[1] + 1) * CHUNK_ROWS
        if end == VEC_ROW:
            for cp in vec:
                cp.wait()
            for j in range(4):
                flat[pl.ds(VEC_ROW + j, 9, stride=4), :] = svd[:, j * LN:(j + 1) * LN]
            for j in range(16):
                flat[pl.ds(VEC_ROW + 36 + j, 1), :] = svf[:, j * LN:(j + 1) * LN]
            flat[pl.ds(VEC_ROW + 52, 12), :] = jnp.zeros((12, LN), F32)
            end = ROWS
        while sent < 16 and window_start(2 * sent + 1) + WIN <= end:
            s0_copy(sent, 0).start()
            sent += 1
            if sent > 1:
                s0_add(sent - 2, 0)
    s0_add(15, 0)
    for i in range(16):
        s0_copy(i, 1).start()

    recv = (r1, r2, r3, r4)
    both = pl.ds(0, 2)

    def rs_copy(k, t):
        o, (row, n), _ = COLORS[k]
        idx = [both] * 4
        for d in o[:t]:
            idx[d] = bits[d]
        idx[o[t]] = 1 - bits[o[t]]
        dst = recv[t].at[(both,) * (3 - t) + (pl.ds(row, n),)]
        return pltpu.make_async_remote_copy(acc.at[tuple(idx) + (pl.ds(row, n),)], dst, rs_s.at[k, t], rs_r.at[k, t],
                                            device_id=partner[o[t]], device_id_type=MESH)

    def rs_add(k, t):
        o, (row, n), _ = COLORS[k]
        idx = [None] * 4
        for d in o[:t + 1]:
            idx[d] = bits[d]
        rest = [d for d in range(4) if d not in o[:t + 1]]
        for combo in range(2 ** len(rest)):
            sub = tuple((combo >> (len(rest) - 1 - j)) & 1 for j in range(len(rest)))
            for j, d in enumerate(rest):
                idx[d] = sub[j]
            acc[tuple(idx) + (pl.ds(row, n),)] += recv[t][sub + (pl.ds(row, n),)]

    rs = {}

    def rs_start(k, t):
        rs[k, t] = rs_copy(k, t)
        rs[k, t].start()

    for k in range(6):
        rs_start(k, 0)
    for i in range(16):
        s0_add(i, 1)
    for k in range(6, NC):
        rs_start(k, 0)
    def rs_take(k, t):
        rs[k, t].wait_recv()
        rs_add(k, t)
        if t < 3:
            rs_start(k, t + 1)

    for t in range(3):
        for k in range(NC):
            rs_take(k, t)

    for cp in mvw:
        cp.wait()

    def rows(sl):
        m_new, v_new, w_new = adam_update(gs[sl, :] / 32.0, ms[sl, :], vs[sl, :], ws[sl, :])
        mo[sl, :] = m_new
        vo[sl, :] = v_new
        wn[sl, :] = w_new
        wg[(c,) + bits + (sl,)] = w_new.astype(BF16)

    def adam(row, n):
        for case in range(4):
            @pl.when(2 * x + c == case)
            def _():
                gs[pl.ds(row, n), :] = acc[bits + (pl.ds(row + 2 * case, n),)]

        def block(i, carry):
            rows(pl.ds(pl.multiple_of(row + i * 16, 16), 16))
            return carry

        lax.fori_loop(0, n // 16, block, 0, unroll=5 if row == 0 else 3)
        if n % 16:
            wg[(c,) + bits + (pl.ds(832, 16),)] = jnp.zeros((16, LN), BF16)
            rows(pl.ds(832, 2))

    outs = []

    def put(pairs):
        for a, b in pairs:
            cp = pltpu.make_async_copy(a, b, out_sem.at[len(outs)])
            cp.start()
            outs.append(cp)

    def ag_idx(k, t, kept):
        o = COLORS[k][0]
        idx = [both] * 4
        for d in o[:t]:
            idx[d] = bits[d]
        if t < 4:
            idx[o[t]] = bits[o[t]] if kept else 1 - bits[o[t]]
        return (c,) + tuple(idx) + (pl.ds(*COLORS[k][2]),)

    def ag_copy(k, t):
        ref = wg.at[ag_idx(k, t, True)]
        return pltpu.make_async_remote_copy(ref, ref, ag_s.at[k, t], ag_r.at[k, t],
                                            device_id=partner[COLORS[k][0][t]], device_id_type=MESH)

    def pc_copy(k, t):
        ref = wg.at[ag_idx(k, t, False)]
        return pltpu.make_async_remote_copy(ref, ref, pc_s.at[k, t], pc_r.at[k, t],
                                            device_id=peer, device_id_type=MESH)

    ag, pc = {}, {}

    def ag_start(k, t):
        ag[k, t] = ag_copy(k, t)
        ag[k, t].start()

    def pc_start(k, t):
        pc[k, t] = pc_copy(k, t)
        pc[k, t].start()

    for k in range(6):
        rs_take(k, 3)
    adam(0, EARLY_ROWS)
    for k in range(6):
        ag_start(k, 3)
    for k in range(6, NC):
        rs_take(k, 3)
    adam(EARLY_ROWS, SHARD - EARLY_ROWS)
    for k in range(6, NC):
        ag_start(k, 3)
    for k in range(NC):
        pc_start(k, 4)
    put(((mo, m_out), (vo, v_out), (wn, w_out)))
    for t in BACK[:3]:
        for k in range(NC):
            ag[k, t].wait_recv()
            ag_start(k, t - 1)
            pc_start(k, t)
    for cp in [rs[key] for key in rs]:
        cp.wait_send()
    for g in range(2):
        for i in range(16):
            s0_copy(i, g).wait_send()
    for part in (range(6), range(6, NC)):
        for k in part:
            ag[k, 0].wait_recv()
            pc_start(k, 0)
        for k in part:
            for t in range(5):
                pc[k, t].wait_recv()
        if part[0] == 0:
            spread(wg, flat, 0, EARLY_ROWS)
    spread(wg, flat, EARLY_ROWS, SHARD - EARLY_ROWS)

    for i, (ref, out) in enumerate(((we, we_out), (wi, wi_out), (wo, wo_out), (wa, wa_out))):
        to_native(flat, ref, (0, 2, 3, 1)[i], 1 if ref is wi else 4)
        put(((ref, out),))
    for j in range(4):
        wvd[:, j * LN:(j + 1) * LN] = flat[pl.ds(VEC_ROW + j, 9, stride=4), :].astype(BF16)
    for j in range(16):
        wvf[:, j * LN:(j + 1) * LN] = flat[pl.ds(VEC_ROW + 36 + j, 1), :].astype(BF16)
    put(((wvd, wvd_out), (wvf, wvf_out)))
    for cp in list(ag.values()) + list(pc.values()):
        cp.wait_send()
    for cp in outs:
        cp.wait()


def comm(*args):
    hbm = pl.BlockSpec(memory_space=pl.ANY)
    shard = jax.ShapeDtypeStruct((SHARD, LN), F32)
    dma = pltpu.SemaphoreType.DMA
    weights = ((VOCAB, D), (FF, D), (D, FF), (FF, D), (9, D), (1, FF))
    return pl.pallas_call(
        comm_kernel,
        out_shape=(shard,) * 3 + tuple(jax.ShapeDtypeStruct(s, BF16) for s in weights),
        in_specs=[hbm] * 9,
        out_specs=(hbm,) * 9,
        scratch_shapes=[
            pltpu.VMEM((RING[0], CHUNK // D, D), F32), pltpu.VMEM((RING[1], CHUNK // FF, FF), F32),
            pltpu.VMEM((9, D), F32), pltpu.VMEM((1, FF), F32),
            pltpu.VMEM((ROWS, LN), F32)]
        + [pltpu.VMEM((2,) * n + (WIN, LN), F32) for n in (4,) + BACK]
        + [pltpu.VMEM((SHARD, LN), F32)] * 7
        + [pltpu.VMEM((2,) * 5 + (WROWS, LN), BF16)]
        + [pltpu.VMEM(s, BF16) for s in weights]
        + [dma((sum(RING) + 2,)), dma((3,)), dma((2, 16)), dma((2, 16))]
        + [dma((NC, 4))] * 4 + [dma((NC, 5))] * 2 + [dma((9,))],
        compiler_params=pltpu.CompilerParams(collective_id=0, has_side_effects=True, vmem_limit_bytes=66_000_000),
        name="comm",
    )(*args)


TM = 1024


def ffn_kernel(tok, act, we, wa, wi, wo, wvd, wvf, m_in, v_in, w_in,
               out, we_out, wa_out, wi_out, wo_out, wvd_out, wvf_out, m_out, v_out, w_out):
    i = pl.program_id(0)

    @pl.when(i == 0)
    def _():
        for a, b in ((wvd, wvd_out), (wvf, wvf_out), (m_in, m_out), (v_in, v_out), (w_in, w_out)):
            b[...] = a[...]

    wa_out[...] = wa[...]
    for a, b in ((we, we_out), (wi, wi_out), (wo, wo_out)):
        n = b.shape[0]
        b[...] = a[pl.ds(pl.multiple_of(i * n, n), n), :]
    lane = lax.broadcasted_iota(jnp.int32, (TM, LN), 1)
    col = jnp.transpose(jnp.broadcast_to(tok[0], (LN, TM)), (1, 0))
    hot = jnp.concatenate([(col == lane + LN * j).astype(F32).astype(BF16) for j in range(VOCAB // LN)], axis=1)
    rows = jnp.dot(hot, we[...], preferred_element_type=F32)
    hidden = (rows * math.sqrt(D) + act[...].astype(F32)).astype(BF16)
    step = 512
    parts = []
    pre = jnp.dot(hidden, wi[:, 0:step], preferred_element_type=F32)
    for f in range(0, FF, step):
        nxt = None
        if f + step < FF:
            nxt = jnp.dot(hidden, wi[:, f + step:f + 2 * step], preferred_element_type=F32)
        parts.append(gelu_tanh(pre + wvf[:, f:f + step].astype(F32)).astype(BF16))
        pre = nxt
    inner = jnp.concatenate(parts, axis=1)
    total = jnp.dot(inner, wo[...], preferred_element_type=F32)
    out[...] = (total + wvd[8:9, :].astype(F32)).astype(BF16)


def ffn(tok, act, *rest):
    tokens = act.shape[0]
    steps = tokens // TM
    row = lambda i: (i, 0)

    def whole(ref):
        return pl.BlockSpec(ref.shape, lambda i: (0, 0))

    def part(ref):
        return pl.BlockSpec((ref.shape[0] // steps, ref.shape[1]), row)

    we, wa, wi, wo, wvd, wvf, m, v, w = rest
    outs = (we, wa, wi, wo, wvd, wvf, m, v, w)
    return pl.pallas_call(
        ffn_kernel,
        grid=(steps,),
        out_shape=(jax.ShapeDtypeStruct(act.shape, BF16),) + tuple(jax.ShapeDtypeStruct(a.shape, a.dtype) for a in outs),
        in_specs=[pl.BlockSpec((1, 1, TM), lambda i: (i, 0, 0)), part(act), whole(we), part(wa), whole(wi), whole(wo)]
        + [whole(a) for a in (wvd, wvf, m, v, w)],
        out_specs=(part(act), part(we), part(wa), part(wi), part(wo)) + tuple(whole(a) for a in (wvd, wvf, m, v, w)),
        compiler_params=pltpu.CompilerParams(vmem_limit_bytes=66_000_000),
        name="ffn",
    )(tok.reshape(steps, 1, TM), act, *rest)


def solution(mesh):
    def device_step(g_emb, g_attn, g_in, g_out, g_vecd, g_vecf, opt_m, opt_v, master, tok_ids, act_in):
        m1, v1, w1, *weights = comm(
            g_emb.reshape(VOCAB, D), g_attn.reshape(FF, D), g_in.reshape(D, FF), g_out.reshape(FF, D),
            g_vecd.reshape(9, D), g_vecf.reshape(1, FF),
            opt_m.reshape(SHARD, LN), opt_v.reshape(SHARD, LN), master.reshape(SHARD, LN))
        y_out, we, wa, wi, wo, wvd, wvf, m_new, v_new, w_new = ffn(tok_ids, act_in, *weights, m1, v1, w1)
        return (m_new.reshape(-1), v_new.reshape(-1), w_new.reshape(-1), we, wa.reshape(1, 4, D, D),
                wi.reshape(1, D, FF), wo.reshape(1, FF, D), wvd.reshape(1, 9, D), wvf, y_out)

    grad_specs = tuple(P(AXES, *([None] * (grad_rank - 1))) for grad_rank in GRAD_RANKS)
    in_specs = grad_specs + (P(AXES), P(AXES), P(AXES), P(AXES), P(AXES, None))
    out_specs = (P(AXES), P(AXES), P(AXES), P(), P(), P(), P(), P(), P(), P(AXES, None))
    return jax.shard_map(device_step, mesh=mesh, in_specs=in_specs, out_specs=out_specs, check_vma=False)
```

```python
import functools
import math

import jax
import jax.numpy as jnp
from jax import lax
from jax.experimental import pallas as pl
from jax.experimental.pallas import tpu as pltpu
from jax.sharding import PartitionSpec as P

LEARN_RATE = 0.002
BETA_ONE = 0.9
BETA_TWO = 0.95
ADAM_EPS = 1e-8
ADAM_STEP = 2
AXES = ("dz", "dy", "dx")
GRAD_RANKS = (3, 5, 4, 4, 4, 3)
MESH = pl.DeviceIdType.MESH
F32, BF16 = jnp.float32, jnp.bfloat16

D, FF, VOCAB, LN = 512, 2048, 512, 128
ROWS = 26688
SHARD = 834
WIN = 840
WROWS = 848
TENSORS = ((0, 512, 512), (2048, 2048, 512), (10240, 512, 2048), (18432, 2048, 512))
VEC_ROW = 26624
X, Y, ZA, ZB = 3, 2, 1, 0
BACK = (3, 2, 1, 0)
ORDERS = ((X, Y, ZA, ZB), (X, Y, ZB, ZA), (Y, X, ZA, ZB), (Y, X, ZB, ZA), (ZA, ZB, X, Y), (ZB, ZA, Y, X))
RS_ROWS = (72, 64, 72, 64, 72, 72, 72, 72, 72, 72, 64, 72)
AG_ROWS = (64, 64, 64, 64, 64, 80, 80, 64, 80, 80, 64, 80)
NC = len(RS_ROWS)
COLORS = tuple((ORDERS[k % len(ORDERS)], (sum(RS_ROWS[:k]), RS_ROWS[k]), (sum(AG_ROWS[:k]), AG_ROWS[k]))
               for k in range(NC))
EARLY_ROWS = sum(AG_ROWS[:6])
GROUPS = ((0, sum(RS_ROWS[:6])), (sum(RS_ROWS[:6]), sum(RS_ROWS[6:])))
CHUNK, CHUNK_ROWS = 131072, 1024
RING = 6, 4


def window_start(s):
    return (s // 4) * 3336 + (s % 4) * 832


def adam_update(grad_vals, opt_m, opt_v, master):
    m_new = BETA_ONE * opt_m + (1.0 - BETA_ONE) * grad_vals
    v_new = BETA_TWO * opt_v + (1.0 - BETA_TWO) * grad_vals * grad_vals
    m_hat = m_new / (1.0 - BETA_ONE ** ADAM_STEP)
    v_hat = v_new / (1.0 - BETA_TWO ** ADAM_STEP)
    w_new = master - LEARN_RATE * m_hat / (jnp.sqrt(v_hat) + ADAM_EPS)
    return m_new, v_new, w_new


def window_start(s):
    return (s // 4) * 3336 + (s % 4) * 832


def gelu_tanh(v):
    c = math.sqrt(2.0 / math.pi)
    half = 0.5 * v
    return half + half * jnp.tanh(v * (c + (c * 0.044715) * (v * v)))


def spread(wg, flat, row, n):
    for s in range(32):
        idx = (s % 2,) + slot(s // 2)
        flat[pl.ds(s * SHARD + row, n), :] = wg[idx + (pl.ds(row, n),)].astype(F32)


def to_native(flat, dst, tensor, unroll):
    base, rows, cols = TENSORS[tensor]
    lanes = cols // LN

    def group(g, carry):
        row = pl.multiple_of(g * 16, 16)
        for j in range(lanes):
            dst[pl.ds(row, 16), j * LN:(j + 1) * LN] = flat[
                pl.ds(base + row * lanes + j, 16, stride=lanes), :].astype(BF16)
        return carry

    lax.fori_loop(0, rows // 16, group, 0, unroll=unroll)


def slot(i):
    z = i // 4
    return (z // 2, (z % 2 + z // 2) % 2, (i // 2) % 2, i % 2)


def comm_kernel(ge, ga, gi, go, gvd, gvf, m_in, v_in, w_in, m_out, v_out, w_out, we_out, wa_out, wi_out, wo_out,
                wvd_out, wvf_out,
                st5, st20, svd, svf, flat, acc, r1, r2, r3, r4, gs, ms, vs, ws, mo, vo, wn, wg, we, wa, wi, wo, wvd, wvf,
                ld_sem, mvw_sem, s0_s, s0_r, rs_s, rs_r, ag_s, ag_r, pc_s, pc_r, out_sem):
    z, y, xc = lax.axis_index("dz"), lax.axis_index("dy"), lax.axis_index("dx")
    x, c = xc // 2, xc % 2
    b1, b0 = z // 2, z % 2
    g0 = (b0 + b1) % 2
    bits = (b1, g0, y, x)
    peer = (z, y, 2 * x + 1 - c)
    partner = ((3 - z, y, xc), (2 * b1 + 1 - b0, y, xc), (z, 1 - y, xc), (z, y, 2 * (1 - x) + c))

    srcs = (ge, ga, gi, go)
    order = [(t, j) for t, (_, rows, cols) in enumerate(TENSORS) for j in range(rows * cols // CHUNK)]
    seq = ([ch for ch in order if ch[0] != 2], [ch for ch in order if ch[0] == 2])
    ring_of = (st5, st20)

    def load(kind, pos):
        t, j = seq[kind][pos]
        rows = CHUNK // TENSORS[t][2]
        at = pos % RING[kind]
        return pltpu.make_async_copy(srcs[t].at[pl.ds(j * rows, rows)], ring_of[kind].at[at],
                                     ld_sem.at[kind * RING[0] + at])

    for kind in range(2):
        for pos in range(RING[kind]):
            load(kind, pos).start()
    vec = [pltpu.make_async_copy(a, b, ld_sem.at[sum(RING) + i]) for i, (a, b) in enumerate(((gvd, svd), (gvf, svf)))]
    mvw = [pltpu.make_async_copy(a, b, mvw_sem.at[i]) for i, (a, b) in enumerate(((m_in, ms), (v_in, vs), (w_in, ws)))]
    for cp in vec + mvw:
        cp.start()

    barrier = pltpu.get_barrier_semaphore()
    for dev in (peer,) + partner:
        pl.semaphore_signal(barrier, inc=1, device_id=dev, device_id_type=MESH)
    pl.semaphore_wait(barrier, 5)

    done = [0, 0]

    def take(ch):
        t, j = ch
        kind = 1 if t == 2 else 0
        pos = done[kind]
        assert seq[kind][pos] == ch
        load(kind, pos).wait()
        base, _, cols = TENSORS[t]
        lanes = cols // LN
        rows = CHUNK // cols
        slot = pos % RING[kind]
        ring = ring_of[kind]

        def group(g, carry):
            row = pl.multiple_of(g * 8, 8)
            out = base + (j * rows + row) * lanes
            for i in range(lanes):
                flat[pl.ds(out + i, 8, stride=lanes), :] = ring[slot, pl.ds(row, 8), i * LN:(i + 1) * LN]
            return carry

        lax.fori_loop(0, rows // 8, group, 0, unroll=4 if lanes == 4 else 1)
        done[kind] += 1
        if pos + RING[kind] < len(seq[kind]):
            load(kind, pos + RING[kind]).start()

    def s0_copy(i, g):
        row, n = GROUPS[g]
        start = pl.multiple_of(window_start(2 * i + 1 - c) + row, 8)
        return pltpu.make_async_remote_copy(flat.at[pl.ds(start, n)], acc.at[slot(i) + (pl.ds(row, n),)],
                                            s0_s.at[g, i], s0_r.at[g, i], device_id=peer, device_id_type=MESH)

    def s0_add(i, g):
        row, n = GROUPS[g]
        s0_copy(i, g).wait_recv()
        start = pl.multiple_of(window_start(2 * i + c) + row, 8)
        acc[slot(i) + (pl.ds(row, n),)] += flat[pl.ds(start, n), :]

    sent = 0
    for ch in order:
        take(ch)
        end = TENSORS[ch[0]][0] + (ch[1] + 1) * CHUNK_ROWS
        if end == VEC_ROW:
            for cp in vec:
                cp.wait()
            for j in range(4):
                flat[pl.ds(VEC_ROW + j, 9, stride=4), :] = svd[:, 0, j * LN:(j + 1) * LN]
            for j in range(16):
                flat[pl.ds(VEC_ROW + 36 + j, 1), :] = svf[:, j * LN:(j + 1) * LN]
            flat[pl.ds(VEC_ROW + 52, 12), :] = jnp.zeros((12, LN), F32)
            end = ROWS
        while sent < 16 and window_start(2 * sent + 1) + WIN <= end:
            s0_copy(sent, 0).start()
            sent += 1
            if sent > 1:
                s0_add(sent - 2, 0)
    s0_add(15, 0)
    for i in range(16):
        s0_copy(i, 1).start()

    recv = (r1, r2, r3, r4)
    both = pl.ds(0, 2)

    def rs_copy(k, t):
        o, (row, n), _ = COLORS[k]
        idx = [both] * 4
        for d in o[:t]:
            idx[d] = bits[d]
        idx[o[t]] = 1 - bits[o[t]]
        dst = recv[t].at[(both,) * (3 - t) + (pl.ds(row, n),)]
        return pltpu.make_async_remote_copy(acc.at[tuple(idx) + (pl.ds(row, n),)], dst, rs_s.at[k, t], rs_r.at[k, t],
                                            device_id=partner[o[t]], device_id_type=MESH)

    def rs_add(k, t):
        o, (row, n), _ = COLORS[k]
        idx = [None] * 4
        for d in o[:t + 1]:
            idx[d] = bits[d]
        rest = [d for d in range(4) if d not in o[:t + 1]]
        for combo in range(2 ** len(rest)):
            sub = tuple((combo >> (len(rest) - 1 - j)) & 1 for j in range(len(rest)))
            for j, d in enumerate(rest):
                idx[d] = sub[j]
            acc[tuple(idx) + (pl.ds(row, n),)] += recv[t][sub + (pl.ds(row, n),)]

    rs = {}

    def rs_start(k, t):
        rs[k, t] = rs_copy(k, t)
        rs[k, t].start()

    for k in range(6):
        rs_start(k, 0)
    for i in range(16):
        s0_add(i, 1)
    for k in range(6, NC):
        rs_start(k, 0)
    def rs_take(k, t):
        rs[k, t].wait_recv()
        rs_add(k, t)
        if t < 3:
            rs_start(k, t + 1)

    for t in range(3):
        for k in range(NC):
            rs_take(k, t)

    for cp in mvw:
        cp.wait()

    def rows(sl):
        m_new, v_new, w_new = adam_update(gs[sl, :] / 32.0, ms[sl, :], vs[sl, :], ws[sl, :])
        mo[sl, :] = m_new
        vo[sl, :] = v_new
        wn[sl, :] = w_new
        wg[(c,) + bits + (sl,)] = w_new.astype(BF16)

    def adam(row, n):
        for case in range(4):
            @pl.when(2 * x + c == case)
            def _():
                gs[pl.ds(row, n), :] = acc[bits + (pl.ds(row + 2 * case, n),)]

        def block(i, carry):
            rows(pl.ds(pl.multiple_of(row + i * 16, 16), 16))
            return carry

        lax.fori_loop(0, n // 16, block, 0, unroll=5 if row == 0 else 3)
        if n % 16:
            wg[(c,) + bits + (pl.ds(832, 16),)] = jnp.zeros((16, LN), BF16)
            rows(pl.ds(832, 2))

    outs = []

    def put(pairs):
        for a, b in pairs:
            cp = pltpu.make_async_copy(a, b, out_sem.at[len(outs)])
            cp.start()
            outs.append(cp)

    def ag_idx(k, t, kept):
        o = COLORS[k][0]
        idx = [both] * 4
        for d in o[:t]:
            idx[d] = bits[d]
        if t < 4:
            idx[o[t]] = bits[o[t]] if kept else 1 - bits[o[t]]
        return (c,) + tuple(idx) + (pl.ds(*COLORS[k][2]),)

    def ag_copy(k, t):
        ref = wg.at[ag_idx(k, t, True)]
        return pltpu.make_async_remote_copy(ref, ref, ag_s.at[k, t], ag_r.at[k, t],
                                            device_id=partner[COLORS[k][0][t]], device_id_type=MESH)

    def pc_copy(k, t):
        ref = wg.at[ag_idx(k, t, False)]
        return pltpu.make_async_remote_copy(ref, ref, pc_s.at[k, t], pc_r.at[k, t],
                                            device_id=peer, device_id_type=MESH)

    ag, pc = {}, {}

    def ag_start(k, t):
        ag[k, t] = ag_copy(k, t)
        ag[k, t].start()

    def pc_start(k, t):
        pc[k, t] = pc_copy(k, t)
        pc[k, t].start()

    for k in range(6):
        rs_take(k, 3)
    adam(0, EARLY_ROWS)
    for k in range(6):
        ag_start(k, 3)
    for k in range(6, NC):
        rs_take(k, 3)
    adam(EARLY_ROWS, SHARD - EARLY_ROWS)
    for k in range(6, NC):
        ag_start(k, 3)
    for k in range(NC):
        pc_start(k, 4)
    put(((mo, m_out), (vo, v_out), (wn, w_out)))
    for t in BACK[:3]:
        for k in range(NC):
            ag[k, t].wait_recv()
            ag_start(k, t - 1)
            pc_start(k, t)
    for cp in [rs[key] for key in rs]:
        cp.wait_send()
    for g in range(2):
        for i in range(16):
            s0_copy(i, g).wait_send()
    for part in (range(6), range(6, NC)):
        for k in part:
            ag[k, 0].wait_recv()
            pc_start(k, 0)
        for k in part:
            for t in range(5):
                pc[k, t].wait_recv()
        if part[0] == 0:
            spread(wg, flat, 0, EARLY_ROWS)
    spread(wg, flat, EARLY_ROWS, SHARD - EARLY_ROWS)

    for i, (ref, out) in enumerate(((we, we_out), (wi, wi_out), (wo, wo_out), (wa, wa_out))):
        to_native(flat, ref, (0, 2, 3, 1)[i], 1 if ref is wi else 4)
        put(((ref, out),))
    for j in range(4):
        wvd[:, j * LN:(j + 1) * LN] = flat[pl.ds(VEC_ROW + j, 9, stride=4), :].astype(BF16)
    for j in range(16):
        wvf[:, j * LN:(j + 1) * LN] = flat[pl.ds(VEC_ROW + 36 + j, 1), :].astype(BF16)
    put(((wvd, wvd_out), (wvf, wvf_out)))
    for cp in list(ag.values()) + list(pc.values()):
        cp.wait_send()
    for cp in outs:
        cp.wait()


def comm(*args):
    hbm = pl.BlockSpec(memory_space=pl.ANY)
    shard = jax.ShapeDtypeStruct((SHARD, LN), F32)
    dma = pltpu.SemaphoreType.DMA
    weights = ((VOCAB, D), (FF, D), (D, FF), (FF, D), (9, D), (1, FF))
    return pl.pallas_call(
        comm_kernel,
        out_shape=(shard,) * 3 + tuple(jax.ShapeDtypeStruct(s, BF16) for s in weights),
        in_specs=[hbm] * 9,
        out_specs=(hbm,) * 9,
        scratch_shapes=[
            pltpu.VMEM((RING[0], CHUNK // D, D), F32), pltpu.VMEM((RING[1], CHUNK // FF, FF), F32),
            pltpu.VMEM((9, 1, D), F32), pltpu.VMEM((1, FF), F32),
            pltpu.VMEM((ROWS, LN), F32)]
        + [pltpu.VMEM((2,) * n + (WIN, LN), F32) for n in (4,) + BACK]
        + [pltpu.VMEM((SHARD, LN), F32)] * 7
        + [pltpu.VMEM((2,) * 5 + (WROWS, LN), BF16)]
        + [pltpu.VMEM(s, BF16) for s in weights]
        + [dma((sum(RING) + 2,)), dma((3,)), dma((2, 16)), dma((2, 16))]
        + [dma((NC, 4))] * 4 + [dma((NC, 5))] * 2 + [dma((9,))],
        compiler_params=pltpu.CompilerParams(collective_id=0, has_side_effects=True, vmem_limit_bytes=66_000_000),
        name="comm",
    )(*args)


TM = 1024


def ffn_kernel(tok, act, we, wa, wi, wo, wvd, wvf, m_in, v_in, w_in,
               out, we_out, wa_out, wi_out, wo_out, wvd_out, wvf_out, m_out, v_out, w_out):
    i = pl.program_id(0)

    @pl.when(i == 0)
    def _():
        for a, b in ((wvd, wvd_out), (wvf, wvf_out), (m_in, m_out), (v_in, v_out), (w_in, w_out)):
            b[...] = a[...]

    wa_out[...] = wa[...]
    for a, b in ((we, we_out), (wi, wi_out), (wo, wo_out)):
        n = b.shape[0]
        b[...] = a[pl.ds(pl.multiple_of(i * n, n), n), :]
    lane = lax.broadcasted_iota(jnp.int32, (TM, LN), 1)
    col = jnp.transpose(jnp.broadcast_to(tok[0], (LN, TM)), (1, 0))
    hot = jnp.concatenate([(col == lane + LN * j).astype(F32).astype(BF16) for j in range(VOCAB // LN)], axis=1)
    rows = jnp.dot(hot, we[...], preferred_element_type=F32)
    hidden = (rows * math.sqrt(D) + act[...].astype(F32)).astype(BF16)
    step = 512
    parts = []
    pre = jnp.dot(hidden, wi[:, 0:step], preferred_element_type=F32)
    for f in range(0, FF, step):
        nxt = None
        if f + step < FF:
            nxt = jnp.dot(hidden, wi[:, f + step:f + 2 * step], preferred_element_type=F32)
        parts.append(gelu_tanh(pre + wvf[:, f:f + step].astype(F32)).astype(BF16))
        pre = nxt
    inner = jnp.concatenate(parts, axis=1)
    total = jnp.dot(inner, wo[...], preferred_element_type=F32)
    out[...] = (total + wvd[8:9, :].astype(F32)).astype(BF16)


def ffn(tok, act, *rest):
    tokens = act.shape[0]
    steps = tokens // TM
    row = lambda i: (i, 0)

    def whole(ref):
        return pl.BlockSpec(ref.shape, lambda i: (0, 0))

    def part(ref):
        return pl.BlockSpec((ref.shape[0] // steps, ref.shape[1]), row)

    we, wa, wi, wo, wvd, wvf, m, v, w = rest
    outs = (we, wa, wi, wo, wvd, wvf, m, v, w)
    return pl.pallas_call(
        ffn_kernel,
        grid=(steps,),
        out_shape=(jax.ShapeDtypeStruct(act.shape, BF16),) + tuple(jax.ShapeDtypeStruct(a.shape, a.dtype) for a in outs),
        in_specs=[pl.BlockSpec((1, 1, TM), lambda i: (i, 0, 0)), part(act), whole(we), part(wa), whole(wi), whole(wo)]
        + [whole(a) for a in (wvd, wvf, m, v, w)],
        out_specs=(part(act), part(we), part(wa), part(wi), part(wo)) + tuple(whole(a) for a in (wvd, wvf, m, v, w)),
        compiler_params=pltpu.CompilerParams(vmem_limit_bytes=66_000_000),
        name="ffn",
    )(tok.reshape(steps, 1, TM), act, *rest)


def solution(mesh):
    def device_step(g_emb, g_attn, g_in, g_out, g_vecd, g_vecf, opt_m, opt_v, master, tok_ids, act_in):
        m1, v1, w1, *weights = comm(
            g_emb.reshape(VOCAB, D), g_attn.reshape(FF, D), g_in.reshape(D, FF), g_out.reshape(FF, D),
            g_vecd.reshape(9, 1, D), g_vecf.reshape(1, FF),
            opt_m.reshape(SHARD, LN), opt_v.reshape(SHARD, LN), master.reshape(SHARD, LN))
        y_out, we, wa, wi, wo, wvd, wvf, m_new, v_new, w_new = ffn(tok_ids, act_in, *weights, m1, v1, w1)
        return (m_new.reshape(-1), v_new.reshape(-1), w_new.reshape(-1), we, wa.reshape(1, 4, D, D),
                wi.reshape(1, D, FF), wo.reshape(1, FF, D), wvd.reshape(1, 9, D), wvf, y_out)

    grad_specs = tuple(P(AXES, *([None] * (grad_rank - 1))) for grad_rank in GRAD_RANKS)
    in_specs = grad_specs + (P(AXES), P(AXES), P(AXES), P(AXES), P(AXES, None))
    out_specs = (P(AXES), P(AXES), P(AXES), P(), P(), P(), P(), P(), P(), P(AXES, None))
    return jax.shard_map(device_step, mesh=mesh, in_specs=in_specs, out_specs=out_specs, check_vma=False)
```
